32 devices in a mesh: srow: 4 (over y, core), scol: 8 (over z, x).
Axes of the slice: x: 2, y: 2, z: 4, core: 2. Of those that a mesh axis runs over, the one named last changes fastest.
Arguments:
- loads: float32 [4, 16, 4, 128], P('srow', 'scol'), may hold values from -6 to 6
- local_inverse: float32 [4, 16, 128, 128], P('srow', 'scol'), as said below
- dirichlet: float32 [4, 16, 128, 128], P('srow', 'scol'), as said below
- corner_coupling: float32 [4, 16, 128], P('srow', 'scol'), may hold values from -4 to 4
- coarse_inverse: float32 [4, 16, 16], P('srow', 'scol'), as said below
- partner: int32 [4, 16, 128], P('srow', 'scol'), may hold values from -1 to 31, as said below
Outputs:
- multipliers: float32 [4, 16, 4, 128], P('srow', 'scol')
- residual: float32 [4, 16, 4, 128], P('srow', 'scol')
The draws below stay inside these ranges and needn't reach their ends.
Inputs may be any that keep to these rules, and one draw needn't show every extreme that they name: `partner`: on each edge of each subdomain the first n entries, for some n of 1 to 32, are the positions 0 to n - 1 in order or reversed, the rest are -1; the two subdomains sharing an edge have the same n and mutually inverse lists. `local_inverse`: each block is symmetric positive definite. `dirichlet`: each block is symmetric positive definite. `coarse_inverse`: each band's matrix is symmetric positive definite.
All inputs are finite; a program needn't handle non-finite values.
Results may differ from the reference program's by a relative error of at most 0.0003.
Values sent between devices are 32-bit elements; how exact they have to be, the bound alone decides.
A program may use at most 64 MiB of HBM per device.

```python
import math
import jax
import jax.numpy as jnp
from jax import lax

NB = 128
SR = 1
SC = 2
NRHS = 4
ITERS = 3
NRS = 4
NCS = 16
BANDS = 4
ORDER = 16
N_SCOL = 8


def symmetric_draw(key, lead, order, diag_low, diag_high):
    key_off = jax.random.fold_in(key, 1)
    key_diag = jax.random.fold_in(key, 2)
    noise = jnp.clip(jax.random.normal(key_off, lead + (order, order), jnp.float32), -4.0, 4.0)
    diagonal = jax.random.uniform(key_diag, lead + (order,), jnp.float32, diag_low, diag_high)
    mixed = (noise + jnp.swapaxes(noise, -1, -2)) * (0.5 / math.sqrt(2.0 * order))
    return mixed + diagonal[..., :, None] * jnp.eye(order, dtype=jnp.float32)


def draw_local_inverse(key, part):
    return symmetric_draw(jax.random.fold_in(key, 5), (NRS, NCS), NB, 1.5, 3.0)


def draw_dirichlet(key, part):
    return symmetric_draw(jax.random.fold_in(key, 7), (NRS, NCS), NB, 1.5, 3.0)


def draw_coarse_inverse(key, part):
    return symmetric_draw(jax.random.fold_in(key, 9), (BANDS,), ORDER, 1.5, 3.0)


def draw_partner(key, part):
    edge_len = NB // 4
    flips = jax.random.randint(jax.random.fold_in(key, 11), (NRS, NCS, 2), 0, 2)
    counts = jax.random.randint(jax.random.fold_in(key, 12), (NRS, NCS, 2), 1, edge_len + 1)
    counts = counts.at[0, 0, 0].set(edge_len).at[0, 0, 1].set(1)
    lengths = jnp.stack([jnp.roll(counts[:, :, 0], 1, axis=1), counts[:, :, 0], jnp.roll(counts[:, :, 1], 1, axis=0), counts[:, :, 1]], axis=-1)
    reversed_edge = jnp.stack([jnp.roll(flips[:, :, 0], 1, axis=1), flips[:, :, 0], jnp.roll(flips[:, :, 1], 1, axis=0), flips[:, :, 1]], axis=-1)
    places = jnp.arange(edge_len, dtype=jnp.int32)
    lengths = lengths[..., None]
    facing = jnp.where(reversed_edge[..., None] == 1, lengths - 1 - places, places)
    listed = jnp.where(places < lengths, facing, -1)
    return listed.reshape(NRS, NCS, NB).astype(jnp.int32)


def block_levels(stream_key, shape, shards, least, high):
    level = 1.0
    for dim, parts in shards:
        draws = jax.random.uniform(jax.random.fold_in(jax.random.fold_in(stream_key, 6), dim), (parts,), jnp.float32, least / len(shards), high / len(shards))
        level = level * jnp.repeat(jnp.exp(draws), shape[dim] // parts).reshape((-1,) + (1,) * (len(shape) - 1 - dim))
    return level


def bell_draw(rng, shape, width, reach, pieces=(), kind=jnp.bfloat16):
    array = jax.random.normal(rng, shape, jnp.float32) * width
    if len(pieces) > 0:
        array = block_levels(rng, shape, pieces, -0.22, 0.18) * array
    return jnp.clip(array, min=-reach, max=reach).astype(kind)


def setup_inputs(seed: int = 0) -> dict:
    arg_keys = jax.random.split(jax.random.key(seed), 7)
    return {
        "loads": bell_draw(arg_keys[0], (NRS, NCS, NRHS, NB), 1.0, 6.0, ((0, 4), (1, 8)), jnp.float32),
        "local_inverse": draw_local_inverse(jax.random.fold_in(arg_keys[6], 71), 0),
        "dirichlet": draw_dirichlet(jax.random.fold_in(arg_keys[6], 71), 0),
        "corner_coupling": bell_draw(arg_keys[3], (NRS, NCS, NB), (3.0 * NB ** -0.5), 4.0, ((0, 4), (1, 8)), jnp.float32),
        "coarse_inverse": draw_coarse_inverse(jax.random.fold_in(arg_keys[6], 71), 0),
        "partner": draw_partner(jax.random.fold_in(arg_keys[6], 71), 0),
    }


precise = lax.Precision.HIGHEST


def jump(values, partner):
    edge_len = NB // 4
    west_side = jnp.roll(values, 1, axis=1)[..., edge_len:2 * edge_len]
    east_side = jnp.roll(values, -1, axis=1)[..., 0:edge_len]
    south_side = jnp.roll(values, 1, axis=0)[..., 3 * edge_len:]
    north_side = jnp.roll(values, -1, axis=0)[..., 2 * edge_len:3 * edge_len]
    facing = jnp.concatenate([west_side, east_side, south_side, north_side], axis=-1)
    offset = (jnp.arange(NB, dtype=jnp.int32) // edge_len) * edge_len
    position = (jnp.clip(partner, 0, edge_len - 1) + offset).astype(jnp.int32)
    position = jnp.broadcast_to(position[:, :, None, :], values.shape)
    picked = jnp.take_along_axis(facing, position, axis=-1)
    return jnp.where(partner[:, :, None, :] >= 0, values - picked, jnp.zeros_like(values))


def jump_transposed(values, partner):
    return jump(values, partner)


def apply_inverse(values, local_inverse, corner_coupling, coarse_inverse):
    blocks = jnp.einsum("ijab,ijrb->ijra", local_inverse, values, precision=precise)
    coarse_in = jnp.einsum("ijb,ijrb->ijr", corner_coupling, values, precision=precise)
    banded = coarse_in.reshape(BANDS, SR, N_SCOL, SC, NRHS).transpose(0, 2, 1, 3, 4).reshape(BANDS, ORDER, NRHS)
    solved = jnp.einsum("bxy,byr->bxr", coarse_inverse, banded, precision=precise)
    coarse_out = solved.reshape(BANDS, N_SCOL, SR, SC, NRHS).transpose(0, 2, 1, 3, 4).reshape(NRS, NCS, NRHS)
    return blocks + corner_coupling[:, :, None, :] * coarse_out[..., None]


def inner(left, right):
    return jnp.sum(left * right, axis=(0, 1, 3))


def scaled(coef, values):
    return coef[None, None, :, None] * values


def reference(loads, local_inverse, dirichlet, corner_coupling, coarse_inverse, partner):
    def operator(values):
        spread = jump_transposed(values, partner)
        return jump(apply_inverse(spread, local_inverse, corner_coupling, coarse_inverse), partner)

    def precond(values):
        spread = jump_transposed(values, partner)
        return jump(jnp.einsum("ijab,ijrb->ijra", dirichlet, spread, precision=precise), partner)

    right = operator(loads)
    multipliers = jnp.zeros_like(right)
    residual = right
    precon = precond(residual)
    search = precon
    gamma = inner(residual, precon)
    for iteration in range(ITERS):
        image = operator(search)
        step_size = gamma / inner(search, image)
        multipliers = multipliers + scaled(step_size, search)
        residual = residual - scaled(step_size, image)
        if iteration + 1 < ITERS:
            precon = precond(residual)
            gamma_new = inner(residual, precon)
            search = precon + scaled(gamma_new / gamma, search)
            gamma = gamma_new
    return multipliers, residual
```

```python
import functools

import jax
import jax.numpy as jnp
from jax import lax
from jax.experimental import pallas as pl
from jax.experimental.pallas import tpu as pltpu
from jax.sharding import PartitionSpec as P

ITERS = 3
MESH = pl.DeviceIdType.MESH
precise = lax.Precision.HIGHEST
NEAR = ((0, 0), (0, 1), (0, -1), (1, 0), (-1, 0))
FAR = ((1, 1), (1, -1), (-1, 1), (-1, -1), (2, 0), (-2, 0))
UNROLL = 64


def slot_list(nr, nc):
    near, slots = [], []
    for offsets, out in ((NEAR, near), (FAR, None)):
        for di, dj in offsets:
            off = (di % nr, dj % nc)
            if off not in slots:
                slots.append(off)
                if out is not None:
                    out.append(off)
    return near, slots


def kernel(nr, nc, near, slots, sc, nrhs, loads_in, cpl_in, cinv_in, part_in, linv, dirich, out,
           loads, cpl, cinv, part, lbuf, dbuf, lpair, dpair, loads_n, part_n, cpl_n, dnear, kc, kt, ub, qb,
           local_sem, k_send, k_recv, c_send, c_recv, l_send, l_recv, p_send, p_recv, d_send, d_recv,
           u_send, u_recv, q_send, q_recv):
    rows, width = loads.shape
    edge = width // 4
    ndev = nr * nc
    ncols = nc * sc
    lanes = kt.shape[-1]
    i, j = lax.axis_index("srow"), lax.axis_index("scol")

    def target(di, dj):
        return (lax.rem(i - di + nr, nr), lax.rem(j - dj + nc, nc))

    def others(step):
        if ndev <= UNROLL:
            far_first = sorted(range(1, ndev), key=lambda k: (-min(k // nc, nr - k // nc), min(k % nc, nc - k % nc) % (nc // 2)))
            for k in far_first:
                step(k, k // nc, k % nc)
        else:
            @pl.loop(1, ndev)
            def _(k):
                step(k, lax.div(k, nc), lax.rem(k, nc))

    barrier = pltpu.get_barrier_semaphore()

    def greet(k, di, dj):
        pl.semaphore_signal(barrier, inc=1, device_id=target(di, dj), device_id_type=MESH)

    others(greet)

    fetches = [
        pltpu.make_async_copy(src, dst, local_sem.at[n])
        for n, (src, dst) in enumerate((
            (cinv_in, cinv), (loads_in, loads), (cpl_in, cpl), (part_in, part),
            (linv, lbuf), (dirich, dbuf),
        ))
    ]
    for fetch in fetches:
        fetch.start()

    row = lax.broadcasted_iota(jnp.int32, (rows, width), 0)
    lane = lax.broadcasted_iota(jnp.int32, (rows, width), 1)
    wrow = lax.broadcasted_iota(jnp.int32, (rows, lanes), 0)
    wlane = lax.broadcasted_iota(jnp.int32, (rows, lanes), 1)
    wrhs = lax.rem(wrow, nrhs)
    wsub = lax.div(wrow, nrhs)
    of_rhs = lax.div(wlane, ncols) == wrhs
    gamma_lane = wlane == nrhs * ncols + wrhs
    curve_lane = wlane == nrhs * ncols + nrhs + wrhs

    def spread(block):
        out = jnp.broadcast_to(block[0:1], (rows, block.shape[1]))
        which = lax.div(lax.broadcasted_iota(jnp.int32, out.shape, 0), nrhs)
        for s in range(1, sc):
            out = jnp.where(which == s, jnp.broadcast_to(block[s : s + 1], out.shape), out)
        return out

    def place(dj):
        column = lax.rem(j + dj, nc) * sc
        return wlane == wrhs * ncols + column + wsub

    def index_of(block):
        partner = spread(block)
        position = jnp.clip(partner, 0, edge - 1) + (edge * (1 - 2 * lax.rem(lax.div(lane, edge), 2)) + lax.div(lane, edge) * edge)
        return position, partner >= 0

    def split(values):
        high = values.astype(jnp.bfloat16)
        return high, (values - high.astype(jnp.float32)).astype(jnp.bfloat16)

    def split_into(pair, blocks):
        for s, block in enumerate(blocks):
            high, low = split(block)
            pair[s * width : (s + 1) * width, 0:width] = high
            pair[s * width : (s + 1) * width, width : 2 * width] = low

    tile_lane = lax.broadcasted_iota(jnp.int32, (ncols, lanes), 1)
    tile_row = lax.broadcasted_iota(jnp.int32, (ncols, lanes), 0)
    tiler = jnp.where(lax.rem(tile_lane, ncols) == tile_row, 1.0, 0.0)
    for fetch in fetches[:4]:
        fetch.wait()
    tiled = jnp.dot(spread(cinv[...]), tiler, precision=precise, preferred_element_type=jnp.float32)
    for s in range(sc):
        kc[0, s : s + 1] = tiled[s * nrhs : s * nrhs + 1]
    kt[0] = jnp.where(of_rhs, tiled, 0.0)

    own_position, own_active = index_of(part[...])
    coupling = spread(cpl[...])
    own_place = place(0)
    pl.semaphore_wait(barrier, ndev - 1)

    def remote(src, dst, send, recv, off):
        copy = pltpu.make_async_remote_copy(
            src_ref=src, dst_ref=dst, send_sem=send, recv_sem=recv,
            device_id=target(*off), device_id_type=MESH)
        copy.start()
        return copy

    load_copies = [remote(loads, loads_n.at[n], l_send.at[n], l_recv.at[n], near[n]) for n in range(1, len(near))]
    part_copies = [remote(part, part_n.at[n], p_send.at[n], p_recv.at[n], near[n]) for n in range(1, len(near))]
    fetches[4].wait()
    split_into(lpair, [lbuf[s] for s in range(sc)])
    for n in range(1, len(near)):
        dpair[n] = jnp.zeros(dpair.shape[1:], jnp.bfloat16)

    cpl_copies = [remote(cpl, cpl_n.at[n], c_send.at[n], c_recv.at[n], slots[n]) for n in range(1, len(slots))]
    east_off, west_off = (0, 1 % nc), (0, nc - 1)
    facing_start = {east_off: 0, west_off: edge, (1 % nr, 0): 2 * edge, (nr - 1, 0): 3 * edge}
    d_copies = []
    for n in range(1, len(near)):
        subs = {east_off: pl.ds(0, 1), west_off: pl.ds(sc - 1, 1)}.get(near[n], pl.ds(0, sc))
        src = dirich.at[subs, pl.ds(facing_start[near[n]], edge)]
        d_copies.append((src, dnear.at[n, subs], d_send.at[n], d_recv.at[n], near[n]))

    def send_k(k, di, dj):
        remote(kc.at[0], kc.at[k], k_send, k_recv, (di, dj))

    others(send_k)
    d_copies = [remote(*args) for args in d_copies]

    def jump(mine, west_tile, east_tile, south, north, lookup):
        position, active = lookup
        west = jnp.where(row < nrhs, pltpu.roll(west_tile, nrhs, 0), pltpu.roll(mine, nrhs, 0))
        east = jnp.where(row >= rows - nrhs, pltpu.roll(east_tile, rows - nrhs, 0), pltpu.roll(mine, rows - nrhs, 0))
        side = lax.div(lane, edge)
        comb = jnp.where(side == 0, east, jnp.where(side == 1, west, jnp.where(side == 2, north, south)))
        facing = jnp.take_along_axis(comb, position, axis=1, mode="promise_in_bounds")
        return jnp.where(active, mine - facing, 0.0)

    def slot_of(di, dj):
        off = (di % nr, dj % nc)
        return slots.index(off) if off in slots else None

    def jump_at(tiles, di, dj, lookup):
        def tile(a, b):
            n = slot_of(a, b)
            return tiles[n] if n is not None and n in tiles else tiles[slot_of(di, dj)]
        return jump(tiles[slot_of(di, dj)], tile(di, dj - 1), tile(di, dj + 1), tile(di - 1, dj), tile(di + 1, dj), lookup)

    def multiply(values, pair, count):
        high, low = split(values)
        stacked = jnp.concatenate([high.astype(jnp.float32), low.astype(jnp.float32)], axis=0)
        sub = lax.rem(lax.div(lax.broadcasted_iota(jnp.int32, stacked.shape, 0), nrhs), sc)
        wide = jnp.concatenate(
            [jnp.where(sub == (s if s < count - 1 else sc - 1), stacked, 0.0) for s in range(count)], axis=1)
        product = jnp.dot(wide.astype(jnp.bfloat16), pair, preferred_element_type=jnp.float32)
        return (product[0:rows, 0:width] + product[rows:, 0:width]) + (product[0:rows, width:] + product[rows:, width:])

    def lane_sum(values):
        return jnp.sum(values, axis=1, keepdims=True)

    def publish(rd, values, dots, wide):
        u = multiply(values, lpair[...], sc)
        ub[rd, 0] = u
        count = len(slots) if wide else len(near)
        for n in range(1, count):
            remote(ub.at[rd, 0], ub.at[rd, n], u_send.at[rd], u_recv.at[rd], slots[n])
        message = jnp.where(own_place, lane_sum(coupling * values), 0.0)
        if dots is not None:
            gamma, factor = dots
            message = jnp.where(gamma_lane, lane_sum(gamma), message)
            message = jnp.where(curve_lane, lane_sum(factor * u), message)
        qb[rd, 0] = jnp.sum(message, axis=0, keepdims=True)

        def send_q(k, di, dj):
            remote(qb.at[rd, 0], qb.at[rd, k], q_send.at[rd], q_recv.at[rd], (di, dj))

        others(send_q)
        return count

    def collect(rd, count, want_dots):
        bytes_q = qb.at[rd, pl.ds(1, ndev - 1)]
        pltpu.make_async_copy(bytes_q, bytes_q, q_recv.at[rd]).wait()
        band = [jnp.broadcast_to(jnp.sum(qb[rd, pl.ds(d * nc, nc)], axis=0), (rows, lanes)) for d in range(nr)]
        cols = {}

        def column(k, d):
            return lane_sum(band[d] * kt[k])

        gamma = curve = None
        if want_dots:
            cross = jnp.zeros((rows, lanes), jnp.float32)
            for d in range(nr):
                total = jnp.zeros((rows, lanes), jnp.float32)
                if ndev <= UNROLL:
                    for e in range(nc):
                        cols[(d, e)] = column(d * nc + e, d)
                        total = total + jnp.where(place(e), cols[(d, e)], 0.0)
                else:
                    def add(e, total):
                        return total + jnp.where(place(e), column(d * nc + e, d), 0.0)
                    total = lax.fori_loop(0, nc, add, total)
                cross = cross + total * band[d]
            everything = functools.reduce(jnp.add, band)
            crossed = jnp.broadcast_to(jnp.sum(cross, axis=0, keepdims=True), (rows, lanes))
            curve = lane_sum(jnp.where(of_rhs, crossed, 0.0) + jnp.where(curve_lane, everything, 0.0))
            gamma = lane_sum(jnp.where(gamma_lane, everything, 0.0))
        bytes_u = ub.at[rd, pl.ds(1, count - 1)]
        pltpu.make_async_copy(bytes_u, bytes_u, u_recv.at[rd]).wait()
        tiles = {}
        for n in range(count):
            off = slots[n]
            if off not in cols:
                cols[off] = column(off[0] * nc + off[1], off[0])
            tiles[n] = ub[rd, n] + couplings[n] * cols[off]
        return tiles, gamma, curve

    for n, copy in enumerate(load_copies):
        copy.wait_recv()
    own_lookup = (own_position, own_active)
    load_tiles = {n: (loads[...] if n == 0 else loads_n[n]) for n in range(len(near))}
    start = jump_at(load_tiles, 0, 0, own_lookup)
    count = publish(0, start, None, True)

    for copy in part_copies:
        copy.wait_recv()
    for copy in cpl_copies:
        copy.wait_recv()
    lookups = [own_lookup] + [index_of(part_n[n]) for n in range(1, len(near))]
    couplings = [coupling] + [spread(cpl_n[n]) for n in range(1, len(slots))]
    bytes_k = kc.at[pl.ds(1, ndev - 1)]
    pltpu.make_async_copy(bytes_k, bytes_k, k_recv).wait()

    def widen(k, di, dj):
        kt[k] = jnp.where(of_rhs, spread(kc[k]), 0.0)

    others(widen)
    fetches[5].wait()
    for copy in d_copies:
        copy.wait_recv()
    east, west = near.index(east_off), near.index(west_off)
    upright = [n for n in range(len(near)) if n not in (east, west)]

    def edge_into(n, s, pair, at):
        first = facing_start[near[n]]
        high, low = split(dnear[n, s].T)
        pair[at * width : (at + 1) * width, first : first + edge] = high
        pair[at * width : (at + 1) * width, width + first : width + first + edge] = low

    split_into(dpair.at[0], [dbuf[s] for s in range(sc)])
    for n in upright[1:]:
        for s in range(sc):
            edge_into(n, s, dpair.at[n], s)
    edge_into(east, 0, dpair.at[east], 0)
    edge_into(west, sc - 1, dpair.at[east], 1)
    tiles, _, _ = collect(0, count, False)
    residual = [jump_at(tiles, *near[n], lookups[n]) for n in range(len(near))]

    multipliers = jnp.zeros((rows, width), jnp.float32)
    search = along = gamma = step_size = None
    for iteration in range(ITERS):
        rd = iteration + 1
        last = rd == ITERS
        weighted = {}
        for n in upright:
            weighted[n] = multiply(2.0 * residual[n], dpair[n], sc)
        beside = jnp.where(row < nrhs, residual[east], residual[west])
        weighted[east] = weighted[west] = multiply(2.0 * beside, dpair[east, pl.ds(0, 2 * width)], 2)
        precon = jump_at(weighted, 0, 0, own_lookup)
        doubled = 2.0 * precon
        count = publish(rd, doubled, (residual[0] * precon, doubled), not last)
        tiles, gamma_new, curve = collect(rd, count, True)
        kept = 1 if last else len(near)
        image = [jump_at(tiles, *near[n], lookups[n]) for n in range(kept)]
        if iteration == 0:
            step_size = gamma_new / curve
            search, along = precon, image
        else:
            ratio = gamma_new / gamma
            step_size = gamma_new / (curve - ratio * gamma_new / step_size)
            search = precon + ratio * search
            along = [image[n] + ratio * along[n] for n in range(kept)]
        gamma = gamma_new
        multipliers = multipliers + step_size * search
        residual = [residual[n] - step_size * along[n] for n in range(kept)]
    out[0] = multipliers
    out[1] = residual[0]

    for copy in load_copies + part_copies + cpl_copies + d_copies:
        copy.wait_send()
    pltpu.make_async_copy(bytes_k, bytes_k, k_send).wait()
    for rd in range(ITERS + 1):
        bytes_q = qb.at[rd, pl.ds(1, ndev - 1)]
        pltpu.make_async_copy(bytes_q, bytes_q, q_send.at[rd]).wait()
        sent = (len(near) if rd == ITERS else len(slots)) - 1
        bytes_u = ub.at[rd, pl.ds(1, sent)]
        pltpu.make_async_copy(bytes_u, bytes_u, u_send.at[rd]).wait()


def solution(mesh):
    nr, nc = mesh.shape["srow"], mesh.shape["scol"]
    near, slots = slot_list(nr, nc)

    def body(loads, local_inverse, dirichlet, corner_coupling, coarse_inverse, partner):
        sr, sc, nrhs, width = loads.shape
        rows = sr * sc * nrhs
        ndev = nr * nc
        lanes = -(-(nrhs * nc * sc + 2 * nrhs) // 128) * 128
        dma = pltpu.SemaphoreType.DMA
        f32 = jnp.float32
        vmem = pl.BlockSpec(memory_space=pltpu.VMEM)
        hbm = pl.BlockSpec(memory_space=pl.ANY)
        rounds = ITERS + 1
        out = pl.pallas_call(
            functools.partial(kernel, nr, nc, near, slots, sc, nrhs),
            out_shape=pltpu.VMEM((2, rows, width), f32),
            in_specs=[hbm] * 6,
            out_specs=vmem,
            scratch_shapes=[
                pltpu.VMEM((rows, width), f32),
                pltpu.VMEM((sc, width), f32),
                pltpu.VMEM((sc, coarse_inverse.shape[-1]), f32),
                pltpu.VMEM((sc, width), jnp.int32),
                pltpu.VMEM((sc, width, width), f32),
                pltpu.VMEM((sc, width, width), f32),
                pltpu.VMEM((sc * width, 2 * width), jnp.bfloat16),
                pltpu.VMEM((len(near), sc * width, 2 * width), jnp.bfloat16),
                pltpu.VMEM((len(near), rows, width), f32),
                pltpu.VMEM((len(near), sc, width), jnp.int32),
                pltpu.VMEM((len(slots), sc, width), f32),
                pltpu.VMEM((len(near), sc, width // 4, width), f32),
                pltpu.VMEM((ndev, sc, lanes), f32),
                pltpu.VMEM((ndev, rows, lanes), f32),
                pltpu.VMEM((rounds, len(slots), rows, width), f32),
                pltpu.VMEM((rounds, ndev, 1, lanes), f32),
                dma((6,)), dma, dma,
                dma((len(slots),)), dma((len(slots),)),
                dma((len(near),)), dma((len(near),)),
                dma((len(near),)), dma((len(near),)),
                dma((len(near),)), dma((len(near),)),
                dma((rounds,)), dma((rounds,)),
                dma((rounds,)), dma((rounds,)),
            ],
            compiler_params=pltpu.CompilerParams(collective_id=0, has_side_effects=True),
        )(
            loads.reshape(rows, width),
            corner_coupling.reshape(sc, width),
            coarse_inverse.reshape(sc, coarse_inverse.shape[-1]),
            partner.reshape(sc, width),
            local_inverse.reshape(sc, width, width),
            dirichlet.reshape(sc, width, width),
        )
        return out[0].reshape(loads.shape), out[1].reshape(loads.shape)

    return jax.shard_map(
        body,
        mesh=mesh,
        in_specs=(
            P("srow", "scol", None, None),
            P("srow", "scol", None, None),
            P("srow", "scol", None, None),
            P("srow", "scol", None),
            P("srow", "scol", None),
            P("srow", "scol", None),
        ),
        out_specs=(P("srow", "scol", None, None), P("srow", "scol", None, None)),
        check_vma=False,
    )
```

```python
import functools

import jax
import jax.numpy as jnp
from jax import lax
from jax.experimental import pallas as pl
from jax.experimental.pallas import tpu as pltpu
from jax.sharding import PartitionSpec as P

ITERS = 3
MESH = pl.DeviceIdType.MESH
precise = lax.Precision.HIGHEST
NEAR = ((0, 0), (0, 1), (0, -1), (1, 0), (-1, 0))
FAR = ((1, 1), (1, -1), (-1, 1), (-1, -1), (2, 0), (-2, 0))
UNROLL = 64


def slot_list(nr, nc):
    near, slots = [], []
    for offsets, out in ((NEAR, near), (FAR, None)):
        for di, dj in offsets:
            off = (di % nr, dj % nc)
            if off not in slots:
                slots.append(off)
                if out is not None:
                    out.append(off)
    return near, slots


def kernel(nr, nc, near, slots, sc, nrhs, loads_in, cpl_in, cinv_in, part_in, linv, dirich, out,
           loads, cpl, cinv, part, lbuf, dbuf, lpair, dpair, loads_n, part_n, cpl_n, dnear, kc, kt, ub, qb,
           local_sem, k_send, k_recv, c_send, c_recv, l_send, l_recv, p_send, p_recv, d_send, d_recv,
           u_send, u_recv, q_send, q_recv):
    rows, width = loads.shape
    edge = width // 4
    ndev = nr * nc
    ncols = nc * sc
    lanes = kt.shape[-1]
    i, j = lax.axis_index("srow"), lax.axis_index("scol")

    def target(di, dj):
        return (lax.rem(i - di + nr, nr), lax.rem(j - dj + nc, nc))

    def others(step):
        if ndev <= UNROLL:
            far_first = sorted(range(1, ndev), key=lambda k: (-min(k // nc, nr - k // nc), min(k % nc, nc - k % nc) % (nc // 2)))
            for k in far_first:
                step(k, k // nc, k % nc)
        else:
            @pl.loop(1, ndev)
            def _(k):
                step(k, lax.div(k, nc), lax.rem(k, nc))

    barrier = pltpu.get_barrier_semaphore()

    def greet(k, di, dj):
        pl.semaphore_signal(barrier, inc=1, device_id=target(di, dj), device_id_type=MESH)

    others(greet)

    fetches = [
        pltpu.make_async_copy(src, dst, local_sem.at[n])
        for n, (src, dst) in enumerate((
            (cinv_in, cinv), (loads_in, loads), (cpl_in, cpl), (part_in, part),
            (linv, lbuf), (dirich, dbuf),
        ))
    ]
    for fetch in fetches:
        fetch.start()

    row = lax.broadcasted_iota(jnp.int32, (rows, width), 0)
    lane = lax.broadcasted_iota(jnp.int32, (rows, width), 1)
    wrow = lax.broadcasted_iota(jnp.int32, (rows, lanes), 0)
    wlane = lax.broadcasted_iota(jnp.int32, (rows, lanes), 1)
    wrhs = lax.rem(wrow, nrhs)
    wsub = lax.div(wrow, nrhs)
    of_rhs = lax.div(wlane, ncols) == wrhs
    gamma_lane = wlane == nrhs * ncols + wrhs
    curve_lane = wlane == nrhs * ncols + nrhs + wrhs

    def spread(block):
        out = jnp.broadcast_to(block[0:1], (rows, block.shape[1]))
        which = lax.div(lax.broadcasted_iota(jnp.int32, out.shape, 0), nrhs)
        for s in range(1, sc):
            out = jnp.where(which == s, jnp.broadcast_to(block[s : s + 1], out.shape), out)
        return out

    def place(dj):
        column = lax.rem(j + dj, nc) * sc
        return wlane == wrhs * ncols + column + wsub

    def index_of(block):
        partner = spread(block)
        position = jnp.clip(partner, 0, edge - 1) + (edge * (1 - 2 * lax.rem(lax.div(lane, edge), 2)) + lax.div(lane, edge) * edge)
        return position, partner >= 0

    def split(values):
        high = values.astype(jnp.bfloat16)
        return high, (values - high.astype(jnp.float32)).astype(jnp.bfloat16)

    def split_into(pair, blocks):
        for s, block in enumerate(blocks):
            high, low = split(block)
            pair[s * width : (s + 1) * width, 0:width] = high
            pair[s * width : (s + 1) * width, width : 2 * width] = low

    tile_lane = lax.broadcasted_iota(jnp.int32, (ncols, lanes), 1)
    tile_row = lax.broadcasted_iota(jnp.int32, (ncols, lanes), 0)
    tiler = jnp.where(lax.rem(tile_lane, ncols) == tile_row, 1.0, 0.0)
    for fetch in fetches[:4]:
        fetch.wait()
    tiled = jnp.dot(spread(cinv[...]), tiler, precision=precise, preferred_element_type=jnp.float32)
    for s in range(sc):
        kc[0, s : s + 1] = tiled[s * nrhs : s * nrhs + 1]
    kt[0] = jnp.where(of_rhs, tiled, 0.0)

    own_position, own_active = index_of(part[...])
    coupling = spread(cpl[...])
    own_place = place(0)
    pl.semaphore_wait(barrier, ndev - 1)

    def remote(src, dst, send, recv, off):
        copy = pltpu.make_async_remote_copy(
            src_ref=src, dst_ref=dst, send_sem=send, recv_sem=recv,
            device_id=target(*off), device_id_type=MESH)
        copy.start()
        return copy

    load_copies = [remote(loads, loads_n.at[n], l_send.at[n], l_recv.at[n], near[n]) for n in range(1, len(near))]
    part_copies = [remote(part, part_n.at[n], p_send.at[n], p_recv.at[n], near[n]) for n in range(1, len(near))]
    fetches[4].wait()
    split_into(lpair, [lbuf[s] for s in range(sc)])
    for n in range(1, len(near)):
        dpair[n] = jnp.zeros(dpair.shape[1:], jnp.bfloat16)

    cpl_copies = [remote(cpl, cpl_n.at[n], c_send.at[n], c_recv.at[n], slots[n]) for n in range(1, len(slots))]
    east_off, west_off = (0, 1 % nc), (0, nc - 1)
    facing_start = {east_off: 0, west_off: edge, (1 % nr, 0): 2 * edge, (nr - 1, 0): 3 * edge}
    d_copies = []
    for n in range(1, len(near)):
        subs = {east_off: pl.ds(0, 1), west_off: pl.ds(sc - 1, 1)}.get(near[n], pl.ds(0, sc))
        src = dirich.at[subs, pl.ds(facing_start[near[n]], edge)]
        d_copies.append((src, dnear.at[n, subs], d_send.at[n], d_recv.at[n], near[n]))

    def send_k(k, di, dj):
        remote(kc.at[0], kc.at[k], k_send, k_recv, (di, dj))

    others(send_k)
    d_copies = [remote(*args) for args in d_copies]

    def jump(mine, west_tile, east_tile, south, north, lookup):
        position, active = lookup
        west = jnp.where(row < nrhs, pltpu.roll(west_tile, nrhs, 0), pltpu.roll(mine, nrhs, 0))
        east = jnp.where(row >= rows - nrhs, pltpu.roll(east_tile, rows - nrhs, 0), pltpu.roll(mine, rows - nrhs, 0))
        side = lax.div(lane, edge)
        comb = jnp.where(side == 0, east, jnp.where(side == 1, west, jnp.where(side == 2, north, south)))
        facing = jnp.take_along_axis(comb, position, axis=1, mode="promise_in_bounds")
        return jnp.where(active, mine - facing, 0.0)

    def slot_of(di, dj):
        off = (di % nr, dj % nc)
        return slots.index(off) if off in slots else None

    def jump_at(tiles, di, dj, lookup):
        def tile(a, b):
            n = slot_of(a, b)
            return tiles[n] if n is not None and n in tiles else tiles[slot_of(di, dj)]
        return jump(tiles[slot_of(di, dj)], tile(di, dj - 1), tile(di, dj + 1), tile(di - 1, dj), tile(di + 1, dj), lookup)

    def multiply(values, pair, count):
        total = values.shape[0]
        high, low = split(values)
        stacked = jnp.concatenate([high.astype(jnp.float32), low.astype(jnp.float32)], axis=0)
        sub = lax.rem(lax.div(lax.broadcasted_iota(jnp.int32, stacked.shape, 0), nrhs), sc)
        wide = jnp.concatenate(
            [jnp.where(sub == (s if s < count - 1 else sc - 1), stacked, 0.0) for s in range(count)], axis=1)
        product = jnp.dot(wide.astype(jnp.bfloat16), pair, preferred_element_type=jnp.float32)
        return (product[0:total, 0:width] + product[total:, 0:width]) + (product[0:total, width:] + product[total:, width:])

    def lane_sum(values):
        return jnp.sum(values, axis=1, keepdims=True)

    def publish(rd, values, u, dots, wide):
        ub[rd, 0] = u
        count = len(slots) if wide else len(near)
        for n in range(1, count):
            remote(ub.at[rd, 0], ub.at[rd, n], u_send.at[rd], u_recv.at[rd], slots[n])
        message = jnp.where(own_place, lane_sum(coupling * values), 0.0)
        if dots is not None:
            gamma, factor = dots
            message = jnp.where(gamma_lane, lane_sum(gamma), message)
            message = jnp.where(curve_lane, lane_sum(factor * u), message)
        qb[rd, 0] = jnp.sum(message, axis=0, keepdims=True)

        def send_q(k, di, dj):
            remote(qb.at[rd, 0], qb.at[rd, k], q_send.at[rd], q_recv.at[rd], (di, dj))

        others(send_q)
        return count

    def collect_tiles(rd, count):
        bytes_u = ub.at[rd, pl.ds(1, count - 1)]
        pltpu.make_async_copy(bytes_u, bytes_u, u_recv.at[rd]).wait()
        return {n: ub[rd, n] for n in range(count)}

    def collect_sums(rd, count, want_dots):
        bytes_q = qb.at[rd, pl.ds(1, ndev - 1)]
        pltpu.make_async_copy(bytes_q, bytes_q, q_recv.at[rd]).wait()
        band = [jnp.broadcast_to(jnp.sum(qb[rd, pl.ds(d * nc, nc)], axis=0), (rows, lanes)) for d in range(nr)]
        cols = {}

        def column(k, d):
            return lane_sum(band[d] * kt[k])

        gamma = curve = None
        if want_dots:
            cross = jnp.zeros((rows, lanes), jnp.float32)
            for d in range(nr):
                total = jnp.zeros((rows, lanes), jnp.float32)
                if ndev <= UNROLL:
                    for e in range(nc):
                        cols[(d, e)] = column(d * nc + e, d)
                        total = total + jnp.where(place(e), cols[(d, e)], 0.0)
                else:
                    def add(e, total):
                        return total + jnp.where(place(e), column(d * nc + e, d), 0.0)
                    total = lax.fori_loop(0, nc, add, total)
                cross = cross + total * band[d]
            everything = functools.reduce(jnp.add, band)
            crossed = jnp.broadcast_to(jnp.sum(cross, axis=0, keepdims=True), (rows, lanes))
            curve = lane_sum(jnp.where(of_rhs, crossed, 0.0) + jnp.where(curve_lane, everything, 0.0))
            gamma = lane_sum(jnp.where(gamma_lane, everything, 0.0))
        for n in range(count):
            off = slots[n]
            if off not in cols:
                cols[off] = column(off[0] * nc + off[1], off[0])
        turned = {}
        for n in range(count):
            wide_col = jnp.broadcast_to(cols[slots[n]], (rows, width))
            for m in range(sc):
                turned[n, m] = pltpu.roll(wide_col, m * nrhs, 0) if m else wide_col
        return turned, gamma, curve

    def precondition(images):
        weighted = {}
        for n in upright:
            weighted[n] = multiply(2.0 * images[n], dpair[n], sc)
        high = lax.rem(lax.broadcasted_iota(jnp.int32, images[east].shape, 0), rows) < nrhs
        beside = jnp.where(high, images[east], images[west])
        weighted[east] = weighted[west] = multiply(2.0 * beside, dpair[east, pl.ds(0, 2 * width)], 2)
        return weighted

    def advance(tiles, keep):
        images = [jump_at(tiles, *near[n], lookups[n]) for n in range(len(near) if keep else 1)]
        if not keep:
            return images[0], None, None
        weighted = precondition(images)
        step = jump_at(weighted, 0, 0, own_lookup)
        return images[0], step, multiply(2.0 * step, lpair[...], sc)

    def coarse(base, table, turned, count):
        for n in range(count):
            for m in range(sc):
                base = base + table[n, m] * turned[n, m]
        return base

    for n, copy in enumerate(load_copies):
        copy.wait_recv()
    own_lookup = (own_position, own_active)
    load_tiles = {n: (loads[...] if n == 0 else loads_n[n]) for n in range(len(near))}
    start = jump_at(load_tiles, 0, 0, own_lookup)
    count = publish(0, start, multiply(start, lpair[...], sc), None, True)

    for copy in part_copies:
        copy.wait_recv()
    for copy in cpl_copies:
        copy.wait_recv()
    lookups = [own_lookup] + [index_of(part_n[n]) for n in range(1, len(near))]
    couplings = [coupling] + [spread(cpl_n[n]) for n in range(1, len(slots))]
    bytes_k = kc.at[pl.ds(1, ndev - 1)]
    pltpu.make_async_copy(bytes_k, bytes_k, k_recv).wait()

    def widen(k, di, dj):
        kt[k] = jnp.where(of_rhs, spread(kc[k]), 0.0)

    others(widen)
    fetches[5].wait()
    for copy in d_copies:
        copy.wait_recv()
    east, west = near.index(east_off), near.index(west_off)
    upright = [n for n in range(len(near)) if n not in (east, west)]

    def edge_into(n, s, pair, at):
        first = facing_start[near[n]]
        high, low = split(dnear[n, s].T)
        pair[at * width : (at + 1) * width, first : first + edge] = high
        pair[at * width : (at + 1) * width, width + first : width + first + edge] = low

    split_into(dpair.at[0], [dbuf[s] for s in range(sc)])
    for n in upright[1:]:
        for s in range(sc):
            edge_into(n, s, dpair.at[n], s)
    edge_into(east, 0, dpair.at[east], 0)
    edge_into(west, sc - 1, dpair.at[east], 1)
    group = nrhs // sc
    wrhs_row = lax.rem(row, nrhs)
    wsub_row = lax.div(row, nrhs)
    nothing = jnp.zeros((rows, width), jnp.float32)
    batches = [list(range(first, min(first + group, len(slots)))) for first in range(0, len(slots), group)]
    basis_images = []
    for batch in batches:
        tiles = {n: nothing for n in range(len(slots))}
        for g, n in enumerate(batch):
            tiles[n] = jnp.where(wrhs_row == g * sc + wsub_row, couplings[n], 0.0)
        basis_images.append([jump_at(tiles, *near[n], lookups[n]) for n in range(len(near))])
    stacked = [jnp.concatenate([images[n] for images in basis_images], axis=0) for n in range(len(near))]
    basis_weighted = precondition(stacked)
    basis_steps = []
    for b in range(len(batches)):
        part_of = {n: basis_weighted[n][b * rows : (b + 1) * rows] for n in range(len(near))}
        basis_steps.append(jump_at(part_of, 0, 0, own_lookup))
    stacked_step = jnp.concatenate(basis_steps, axis=0)
    stacked_u = multiply(2.0 * stacked_step, lpair[...], sc)

    def table_of(stack, count):
        table = {}
        for n in range(count):
            first = (n // group) * rows + (n % group) * sc
            for m in range(sc):
                value = None
                for s in range(sc):
                    at = first + s * nrhs + (s - m) % sc
                    line = jnp.broadcast_to(stack[at : at + 1], (rows, width))
                    value = line if value is None else jnp.where(wsub_row == s, line, value)
                table[n, m] = value
        return table

    image_table = table_of(stacked[0], len(near))
    step_table = table_of(stacked_step, len(slots))
    u_table = table_of(stacked_u, len(slots))

    image, step, lifted = advance(collect_tiles(0, count), True)
    turned, _, _ = collect_sums(0, count, False)
    residual = coarse(image, image_table, turned, len(near))
    precon = coarse(step, step_table, turned, len(slots))
    u = coarse(lifted, u_table, turned, len(slots))

    multipliers = jnp.zeros((rows, width), jnp.float32)
    search = along = steps = lifts = gamma = step_size = None
    for iteration in range(ITERS):
        rd = iteration + 1
        last = rd == ITERS
        doubled = 2.0 * precon
        count = publish(rd, doubled, u, (residual * precon, doubled), not last)
        image, step, lifted = advance(collect_tiles(rd, count), not last)
        turned, gamma_new, curve = collect_sums(rd, count, True)
        image = coarse(image, image_table, turned, len(near))
        if not last:
            step = coarse(step, step_table, turned, len(slots))
            lifted = coarse(lifted, u_table, turned, len(slots))
        if iteration == 0:
            step_size = gamma_new / curve
            search, along, steps, lifts = precon, image, step, lifted
        else:
            ratio = gamma_new / gamma
            step_size = gamma_new / (curve - ratio * gamma_new / step_size)
            search = precon + ratio * search
            along = image + ratio * along
            if not last:
                steps = step + ratio * steps
                lifts = lifted + ratio * lifts
        gamma = gamma_new
        multipliers = multipliers + step_size * search
        residual = residual - step_size * along
        if not last:
            precon = precon - step_size * steps
            u = u - step_size * lifts
    out[0] = multipliers
    out[1] = residual

    for copy in load_copies + part_copies + cpl_copies + d_copies:
        copy.wait_send()
    pltpu.make_async_copy(bytes_k, bytes_k, k_send).wait()
    for rd in range(ITERS + 1):
        bytes_q = qb.at[rd, pl.ds(1, ndev - 1)]
        pltpu.make_async_copy(bytes_q, bytes_q, q_send.at[rd]).wait()
        sent = (len(near) if rd == ITERS else len(slots)) - 1
        bytes_u = ub.at[rd, pl.ds(1, sent)]
        pltpu.make_async_copy(bytes_u, bytes_u, u_send.at[rd]).wait()


def solution(mesh):
    nr, nc = mesh.shape["srow"], mesh.shape["scol"]
    near, slots = slot_list(nr, nc)

    def body(loads, local_inverse, dirichlet, corner_coupling, coarse_inverse, partner):
        sr, sc, nrhs, width = loads.shape
        rows = sr * sc * nrhs
        ndev = nr * nc
        lanes = -(-(nrhs * nc * sc + 2 * nrhs) // 128) * 128
        dma = pltpu.SemaphoreType.DMA
        f32 = jnp.float32
        vmem = pl.BlockSpec(memory_space=pltpu.VMEM)
        hbm = pl.BlockSpec(memory_space=pl.ANY)
        rounds = ITERS + 1
        out = pl.pallas_call(
            functools.partial(kernel, nr, nc, near, slots, sc, nrhs),
            out_shape=pltpu.VMEM((2, rows, width), f32),
            in_specs=[hbm] * 6,
            out_specs=vmem,
            scratch_shapes=[
                pltpu.VMEM((rows, width), f32),
                pltpu.VMEM((sc, width), f32),
                pltpu.VMEM((sc, coarse_inverse.shape[-1]), f32),
                pltpu.VMEM((sc, width), jnp.int32),
                pltpu.VMEM((sc, width, width), f32),
                pltpu.VMEM((sc, width, width), f32),
                pltpu.VMEM((sc * width, 2 * width), jnp.bfloat16),
                pltpu.VMEM((len(near), sc * width, 2 * width), jnp.bfloat16),
                pltpu.VMEM((len(near), rows, width), f32),
                pltpu.VMEM((len(near), sc, width), jnp.int32),
                pltpu.VMEM((len(slots), sc, width), f32),
                pltpu.VMEM((len(near), sc, width // 4, width), f32),
                pltpu.VMEM((ndev, sc, lanes), f32),
                pltpu.VMEM((ndev, rows, lanes), f32),
                pltpu.VMEM((rounds, len(slots), rows, width), f32),
                pltpu.VMEM((rounds, ndev, 1, lanes), f32),
                dma((6,)), dma, dma,
                dma((len(slots),)), dma((len(slots),)),
                dma((len(near),)), dma((len(near),)),
                dma((len(near),)), dma((len(near),)),
                dma((len(near),)), dma((len(near),)),
                dma((rounds,)), dma((rounds,)),
                dma((rounds,)), dma((rounds,)),
            ],
            compiler_params=pltpu.CompilerParams(collective_id=0, has_side_effects=True),
        )(
            loads.reshape(rows, width),
            corner_coupling.reshape(sc, width),
            coarse_inverse.reshape(sc, coarse_inverse.shape[-1]),
            partner.reshape(sc, width),
            local_inverse.reshape(sc, width, width),
            dirichlet.reshape(sc, width, width),
        )
        return out[0].reshape(loads.shape), out[1].reshape(loads.shape)

    return jax.shard_map(
        body,
        mesh=mesh,
        in_specs=(
            P("srow", "scol", None, None),
            P("srow", "scol", None, None),
            P("srow", "scol", None, None),
            P("srow", "scol", None),
            P("srow", "scol", None),
            P("srow", "scol", None),
        ),
        out_specs=(P("srow", "scol", None, None), P("srow", "scol", None, None)),
        check_vma=False,
    )
```

```python
import functools

import jax
import jax.numpy as jnp
from jax import lax
from jax.experimental import pallas as pl
from jax.experimental.pallas import tpu as pltpu
from jax.sharding import PartitionSpec as P

ITERS = 3
MESH = pl.DeviceIdType.MESH
precise = lax.Precision.HIGHEST
UNROLL = 64
EAST, WEST, SOUTH, NORTH = 2, 4, 6, 7


def block_slots(nb, nc):
    slots = []
    for dp, dj in ((0, 0), (0, 1), (0, -1), (1, 1), (1, -1), (-1, 1), (-1, -1), (1, 0), (-1, 0)):
        off = (dp % nb, dj % nc)
        if off not in slots:
            slots.append(off)
    return slots


def kernel(nr, nc, slots, sc, nrhs, loads_in, cpl_in, cinv_in, part_in, linv, dirich, out,
           cinv, loads, cpl, part, lbuf, dbuf, lpair, dpair, fpair, loads_n, part_n, cpl_n, dside, dflat, kc, kt, ub, qb,
           local_sem, send_sem, recv_sem, u_send, u_recv, q_send, q_recv):
    rows, width = loads_n.shape[1:]
    edge = width // 4
    ndev = nr * nc
    nb = nr // 2
    nblocks = nb * nc
    ncols = nc * sc
    lanes = kt.shape[-1]
    i, j = lax.axis_index("srow"), lax.axis_index("scol")
    p, core = lax.div(i, 2), lax.rem(i, 2)
    near = [(0, 0), (1, 0), (0, 1), (1, 1), (0, nc - 1), (1, nc - 1), (nr - 1, 0), (2, 0)]
    LOADS, PART, CPL, LINV, DIRICH, SIDE, FLAT, KROW = range(8)

    def others(step):
        if ndev <= UNROLL:
            far_first = sorted(range(1, ndev), key=lambda k: (-min(k // nc, nr - k // nc), min(k % nc, nc - k % nc) % (nc // 2)))
            for k in far_first:
                step(lax.rem(i + k // nc, nr), lax.rem(j + k % nc, nc))
        else:
            @pl.loop(1, ndev)
            def _(k):
                step(lax.rem(i + lax.div(k, nc), nr), lax.rem(j + lax.rem(k, nc), nc))

    barrier = pltpu.get_barrier_semaphore()

    def greet(ti, tj):
        pl.semaphore_signal(barrier, inc=1, device_id=(ti, tj), device_id_type=MESH)

    others(greet)

    fetches = [
        pltpu.make_async_copy(src, dst, local_sem.at[n])
        for n, (src, dst) in enumerate((
            (cinv_in, cinv), (loads_in, loads), (cpl_in, cpl), (part_in, part),
            (linv, lbuf.at[core]), (dirich, dbuf.at[core]),
        ))
    ]
    for fetch in fetches:
        fetch.start()

    row = lax.broadcasted_iota(jnp.int32, (rows, width), 0)
    lane = lax.broadcasted_iota(jnp.int32, (rows, width), 1)
    wrow = lax.broadcasted_iota(jnp.int32, (rows, lanes), 0)
    wlane = lax.broadcasted_iota(jnp.int32, (rows, lanes), 1)
    wrhs = lax.rem(wrow, nrhs)
    wsub = lax.div(wrow, nrhs)
    of_rhs = lax.div(wlane, ncols) == wrhs
    gamma_lane = wlane == nrhs * ncols + wrhs
    curve_lane = wlane == nrhs * ncols + nrhs + wrhs
    rhs_row = lax.rem(row, nrhs)
    sub_row = lax.div(row, nrhs)

    def spread(block):
        out = jnp.broadcast_to(block[0:1], (rows, block.shape[1]))
        which = lax.div(lax.broadcasted_iota(jnp.int32, out.shape, 0), nrhs)
        for s in range(1, sc):
            out = jnp.where(which == s, jnp.broadcast_to(block[s : s + 1], out.shape), out)
        return out

    def place(dj):
        column = lax.rem(j + dj, nc) * sc
        return wlane == wrhs * ncols + column + wsub

    def pick(values, index):
        return jnp.take_along_axis(values, index, axis=1, mode="promise_in_bounds")

    side = lax.div(lane, edge)
    half = lax.rem(side, 2)

    def odd(dr):
        return lax.rem(sub_row + dr, 2)

    def split(values):
        high = values.astype(jnp.bfloat16)
        return high, (values - high.astype(jnp.float32)).astype(jnp.bfloat16)

    def split_into(pair, blocks):
        for s, block in enumerate(blocks):
            high, low = split(block)
            pair[s * width : (s + 1) * width, 0:width] = high
            pair[s * width : (s + 1) * width, width : 2 * width] = low

    tile_lane = lax.broadcasted_iota(jnp.int32, (ncols, lanes), 1)
    tile_row = lax.broadcasted_iota(jnp.int32, (ncols, lanes), 0)
    tiler = jnp.where(lax.rem(tile_lane, ncols) == tile_row, 1.0, 0.0)
    for fetch in fetches[:4]:
        fetch.wait()
    tiled = jnp.dot(spread(cinv[...]), tiler, precision=precise, preferred_element_type=jnp.float32)
    for s in range(sc):
        kc[core * nc, s : s + 1] = tiled[s * nrhs : s * nrhs + 1]
    own_place = place(0)
    partner = spread(part[...])
    other = edge * (1 - 2 * half)
    mirrored = jnp.where((half == 1) & (partner >= 0), partner + side * edge, lane)
    crossed_over = jnp.where(half == 0, pltpu.roll(mirrored, width - edge, 1), pltpu.roll(mirrored, edge, 1))
    own_odd = odd(core)
    forward = jnp.where(own_odd == 1, crossed_over, mirrored)
    backward = jnp.where(own_odd == 1, mirrored + other, mirrored)
    loads_n[core] = pick(loads[...], forward)
    active_own = pick(jnp.where(partner >= 0, 1.0, 0.0), forward)
    coupling_own = pick(spread(cpl[...]), forward)
    for s in range(sc):
        part_n[core, s : s + 1] = active_own[s * nrhs : s * nrhs + 1]
        cpl_n[core, s : s + 1] = coupling_own[s * nrhs : s * nrhs + 1]

    def reorder(buffer):
        for s in range(sc):
            index = jnp.broadcast_to(forward[s * nrhs : s * nrhs + 1], (width, width))
            buffer[core, s] = pick(pick(buffer[core, s], index).T, index)

    pl.semaphore_wait(barrier, ndev - 1)

    def push(src, dst, what, ti, tj):
        pltpu.make_async_remote_copy(
            src_ref=src, dst_ref=dst, send_sem=send_sem.at[what], recv_sem=recv_sem.at[what],
            device_id=(ti, tj), device_id_type=MESH).start()

    west_j, east_j = lax.rem(j + nc - 1, nc), lax.rem(j + 1, nc)
    beyond = lax.rem(p + 2 * core - 1 + nb, nb)
    partner_i = i + 1 - 2 * core
    around = [(EAST + core, 2 * p + t, west_j) for t in range(2)] + [(WEST + core, 2 * p + t, east_j) for t in range(2)]
    around += [(NORTH - core, 2 * beyond + t, j) for t in range(2)]
    toward = around + [(core, partner_i, j)]
    for n, ti, tj in toward:
        push(loads_n.at[core], loads_n.at[n], LOADS, ti, tj)
    for n, ti, tj in toward:
        push(part_n.at[core], part_n.at[n], PART, ti, tj)
    for n, (dp, dj) in enumerate(slots):
        for t in range(2):
            ti, tj = 2 * lax.rem(p - dp + nb, nb) + t, lax.rem(j - dj + nc, nc)
            if (dp, dj) == (0, 0):
                if t == 0:
                    push(cpl_n.at[core], cpl_n.at[core], CPL, partner_i, j)
            else:
                push(cpl_n.at[core], cpl_n.at[2 * n + core], CPL, ti, tj)
    def send_k(ti, tj):
        slot = lax.rem(i - 2 * lax.div(ti, 2) + nr, nr) * nc + lax.rem(j - tj + nc, nc)
        push(kc.at[core * nc], kc.at[slot], KROW, ti, tj)

    others(send_k)
    fetches[4].wait()
    reorder(lbuf)
    push(lbuf.at[core], lbuf.at[core], LINV, partner_i, j)
    fetches[5].wait()
    reorder(dbuf)

    def facing_rows(s, group):
        return dbuf.at[core, s, pl.ds(pl.multiple_of(group * edge, edge), edge)]

    for n, ti, tj in around[:2]:
        push(facing_rows(0, lax.rem(core, 2)), dside.at[core], SIDE, ti, tj)
    for n, ti, tj in around[2:4]:
        push(facing_rows(sc - 1, 1 - lax.rem(core + sc - 1, 2)), dside.at[2 + core], SIDE, ti, tj)
    for n, ti, tj in around[4:]:
        for s in range(sc):
            push(facing_rows(s, 2 + s % 2), dflat.at[1 - core, s], FLAT, ti, tj)
    push(dbuf.at[core], dbuf.at[core], DIRICH, partner_i, j)

    arrivals = {
        LOADS: loads_n.at[pl.ds(0, 7)], PART: part_n.at[pl.ds(0, 7)], CPL: cpl_n.at[pl.ds(0, 2 * len(slots) - 1)],
        LINV: lbuf.at[0], DIRICH: dbuf.at[0], SIDE: dside, FLAT: dflat, KROW: kc.at[pl.ds(0, ndev - 1)],
    }

    def arrived(what):
        pltpu.make_async_copy(arrivals[what], arrivals[what], recv_sem.at[what]).wait()

    def left(what):
        pltpu.make_async_copy(arrivals[what], arrivals[what], send_sem.at[what]).wait()

    def meet(mine, before, after, south, north, dr, active):
        if rows == 2 * nrhs:
            lateral = pltpu.roll(jnp.where(half == odd(dr + 1), before, after), nrhs, 0)
        else:
            lateral = jnp.where(half == odd(dr), pltpu.roll(before, nrhs, 0), pltpu.roll(after, rows - nrhs, 0))
        facing = jnp.where(side < 2, lateral, jnp.where(half == odd(dr), south, north))
        return jnp.where(active, mine - facing, 0.0)

    def jump(mine, west_tile, east_tile, south, north, dr, active):
        before = jnp.where(row < rows - nrhs, mine, west_tile)
        after = jnp.where(row < nrhs, east_tile, mine)
        return meet(mine, before, after, south, north, dr, active)

    def key(dr, dj):
        return (dr % nr, dj % nc)

    def jump_at(tiles, dr, dj, lookup):
        mine = tiles[key(dr, dj)]
        beyond = [tiles.get(key(*at), mine) for at in ((dr, dj - 1), (dr, dj + 1), (dr - 1, dj), (dr + 1, dj))]
        return jump(mine, *beyond, dr, lookup)

    def multiply(values, pair):
        total = values.shape[0]
        high, low = split(values)
        stacked = jnp.concatenate([high.astype(jnp.float32), low.astype(jnp.float32)], axis=0)
        sub = lax.rem(lax.div(lax.broadcasted_iota(jnp.int32, stacked.shape, 0), nrhs), sc)
        wide = jnp.concatenate([jnp.where(sub == s, stacked, 0.0) for s in range(sc)], axis=1)
        product = jnp.dot(wide.astype(jnp.bfloat16), pair, preferred_element_type=jnp.float32)
        return (product[0:total, 0:width] + product[total:, 0:width]) + (product[0:total, width:] + product[total:, width:])

    def lane_sum(values):
        return jnp.sum(values, axis=1, keepdims=True)

    keys = {key(2 * dp + a, dj): (n, a) for n, (dp, dj) in enumerate(slots) for a in range(2)}

    def reach(a, at):
        return min((at[0] - a) % nr, (a - at[0]) % nr) + min(at[1], nc - at[1])

    def flip(index, mask):
        for bit in range(mask.bit_length()):
            if mask >> bit & 1:
                index = index + (1 << bit) - (2 << bit) * lax.rem(lax.div(index, 1 << bit), 2)
        return index

    powers = nb & (nb - 1) == 0 and nc & (nc - 1) == 0
    masks = sorted(((a, b) for a in range(nb) for b in range(nc) if a or b), key=lambda m: -(m[0] + m[1] // 2 + m[1] % 2))

    def q_target(tp, tj):
        return lax.rem(p - tp + nb, nb) * nc + lax.rem(j - tj + nc, nc), 2 * tp + 1 - core, tj

    q_targets = []
    if nblocks <= UNROLL:
        for a, b in masks:
            q_targets.append(q_target(flip(p, a), flip(j, b)) if powers else q_target(lax.rem(p + a, nb), lax.rem(j + b, nc)))
    u_targets = [
        (n, 2 * lax.rem(p - dp + nb, nb) + 1 - core, lax.rem(j - dj + nc, nc)) for n, (dp, dj) in enumerate(slots) if n
    ]
    u_targets.sort(key=lambda target: (slots[target[0]][1] == 0, slots[target[0]][0] == 0))

    def publish(rd, values, u, dots):
        for a in range(2):
            ub[rd, 0, a] = u[a]

        def across(src, dst, send, recv, ti, tj):
            pltpu.make_async_remote_copy(
                src_ref=src, dst_ref=dst, send_sem=send.at[rd], recv_sem=recv.at[rd],
                device_id=(ti, tj), device_id_type=MESH).start()

        for n, ti, tj in u_targets:
            across(ub.at[rd, 0], ub.at[rd, n], u_send, u_recv, ti, tj)
        for a in range(2):
            message = jnp.where(own_place, lane_sum(couplings[a, 0] * values[a]), 0.0)
            if dots is not None and a == 0:
                gamma, curve = dots
                message = jnp.where(gamma_lane, lane_sum(gamma), message)
                message = jnp.where(curve_lane, lane_sum(curve), message)
            qb[rd, 0, a : a + 1] = jnp.sum(message, axis=0, keepdims=True)
        if nblocks <= UNROLL:
            for slot, ti, tj in q_targets:
                across(qb.at[rd, 0], qb.at[rd, slot], q_send, q_recv, ti, tj)
        else:
            @pl.loop(1, nblocks)
            def _(k):
                slot, ti, tj = q_target(lax.rem(p + lax.div(k, nc), nb), lax.rem(j + lax.rem(k, nc), nc))
                across(qb.at[rd, 0], qb.at[rd, slot], q_send, q_recv, ti, tj)

    def sent(rd):
        bytes_q = qb.at[rd, pl.ds(1, nblocks - 1)]
        pltpu.make_async_copy(bytes_q, bytes_q, q_send.at[rd]).wait()
        bytes_u = ub.at[rd, pl.ds(1, len(slots) - 1)]
        pltpu.make_async_copy(bytes_u, bytes_u, u_send.at[rd]).wait()

    def collect_tiles(rd):
        bytes_u = ub.at[rd, pl.ds(1, len(slots) - 1)]
        pltpu.make_async_copy(bytes_u, bytes_u, u_recv.at[rd]).wait()
        bytes_q = qb.at[rd, pl.ds(1, nblocks - 1)]
        pltpu.make_async_copy(bytes_q, bytes_q, q_recv.at[rd]).wait()
        return {at: ub[rd, n, a] for at, (n, a) in keys.items()}

    def collect_sums(rd, want_dots):
        sums = [jnp.sum(qb[rd, pl.ds(d * nc, nc)], axis=0) for d in range(nb)]
        band = [jnp.broadcast_to(sums[d // 2][d % 2 : d % 2 + 1], (rows, lanes)) for d in range(nr)]
        cols = {}

        def column(k, d):
            return lane_sum(band[d] * kt[k])

        gamma = curve = None
        if want_dots:
            cross = jnp.zeros((rows, lanes), jnp.float32)
            for d in range(nr):
                total = jnp.zeros((rows, lanes), jnp.float32)
                if ndev <= UNROLL:
                    for e in range(nc):
                        cols[(d, e)] = column(d * nc + e, d)
                        total = total + jnp.where(place(e), cols[(d, e)], 0.0)
                else:
                    def add(e, total):
                        return total + jnp.where(place(e), column(d * nc + e, d), 0.0)
                    total = lax.fori_loop(0, nc, add, total)
                cross = cross + total * band[d]
            everything = functools.reduce(jnp.add, band)
            crossed = jnp.broadcast_to(jnp.sum(cross, axis=0, keepdims=True), (rows, lanes))
            curve = lane_sum(jnp.where(of_rhs, crossed, 0.0) + jnp.where(curve_lane, everything, 0.0))
            gamma = lane_sum(jnp.where(gamma_lane, everything, 0.0))
        turned = {}
        for at in keys:
            if at not in cols:
                cols[at] = column(at[0] * nc + at[1], at[0])
            wide_col = jnp.broadcast_to(cols[at], (rows, width))
            for m in range(sc):
                turned[at, m] = pltpu.roll(wide_col, m * nrhs, 0) if m else wide_col
        return turned, gamma, curve

    def beside(a):
        return [key(a, 1), key(2, 0) if a else key(-1, 0)]

    def precondition(images):
        weighted = []
        for a in range(2):
            total = images[key(a, 0)].shape[0]
            ring = multiply(2.0 * jnp.concatenate([images[at] for at in beside(a)], axis=0), fpair[a])
            weighted.append({at: ring[m * total : (m + 1) * total] for m, at in enumerate(beside(a))})
            weighted[a][key(a, -1)] = weighted[a][key(a, 1)]
        for a in range(2):
            mine = multiply(2.0 * images[key(a, 0)], dpair[a])
            for ring in weighted:
                ring[key(a, 0)] = mine
        return weighted

    def jump_sides(tiles, a):
        east, mine, west = (tiles[key(a, dj)] for dj in (1, 0, -1))
        before = jnp.where(row < rows - nrhs, west, mine)
        after = jnp.where(row < nrhs, mine, east)
        flat = [jnp.where(row < nrhs, tiles.get(key(a + d, 1), east), tiles.get(key(a + d, -1), west)) for d in (-1, 1)]
        return meet(jnp.where(row < nrhs, east, west), before, after, *flat, a, side_lookups[a])

    def images_of(tiles):
        images = {key(*near[n]): jump_at(tiles, *near[n], lookups[n]) for n in (0, 1, SOUTH, NORTH)}
        for a in range(2):
            images[key(a, 1)] = jump_sides(tiles, a)
        return images

    def advance(tiles, keep):
        if not keep:
            return [jump_at(tiles, a, 0, lookups[a]) for a in range(2)], None, None
        images = images_of(tiles)
        weighted = precondition(images)
        step = [jump_at(weighted[a], a, 0, lookups[a]) for a in range(2)]
        return [images[key(a, 0)] for a in range(2)], step, [multiply(2.0 * step[a], lpair[a]) for a in range(2)]

    def coarse(base, table, turned):
        out = []
        for a in range(2):
            value = base[a]
            for at, m in table[a]:
                value = value + table[a][at, m] * turned[at, m]
            out.append(value)
        return out

    arrived(LINV)
    for a in range(2):
        split_into(lpair.at[a], [lbuf[a, s] for s in range(sc)])
        fpair[a] = jnp.zeros(fpair.shape[1:], jnp.bfloat16)

    arrived(PART)
    partners = [spread(part_n[n]) for n in range(len(near))]
    lookups = [partner > 0.5 for partner in partners]
    side_lookups = [jnp.where(row < nrhs, partners[EAST + a], partners[WEST + a]) > 0.5 for a in range(2)]
    arrived(CPL)
    couplings = {at: spread(cpl_n[2 * n + a]) for at, (n, a) in keys.items()}
    arrived(LOADS)
    load_tiles = {key(*at): loads_n[n] for n, at in enumerate(near)}
    start = [jump_at(load_tiles, a, 0, lookups[a]) for a in range(2)]
    publish(0, start, [multiply(start[a], lpair[a]) for a in range(2)], None)

    arrived(SIDE)
    arrived(FLAT)
    arrived(DIRICH)

    def edge_into(block, a, s, first):
        high, low = split(block.T)
        fpair[a, s * width : (s + 1) * width, first : first + edge] = high
        fpair[a, s * width : (s + 1) * width, width + first : width + first + edge] = low

    for a in range(2):
        split_into(dpair.at[a], [dbuf[a, s] for s in range(sc)])
        edge_into(dside[a], a, 0, edge * (1 - (a + sc - 1) % 2))
        edge_into(dside[2 + a], a, sc - 1, edge * (a % 2))
        for s in range(sc):
            edge_into(dflat[a, s], a, s, edge * (2 + s % 2))

    group = nrhs // sc
    order = list(keys)
    nothing = jnp.zeros((rows, width), jnp.float32)
    batches = [order[first : first + group] for first in range(0, len(order), group)]
    basis_images = []
    for batch in batches:
        tiles = {at: nothing for at in order}
        for g, at in enumerate(batch):
            tiles[at] = jnp.where(rhs_row == g * sc + sub_row, couplings[at], 0.0)
        basis_images.append(images_of(tiles))
    stacked = {at: jnp.concatenate([images[at] for images in basis_images], axis=0) for at in basis_images[0]}
    basis_weighted = precondition(stacked)
    stacked_steps = []
    for a in range(2):
        parts = [
            jump_at({at: basis_weighted[a][at][b * rows : (b + 1) * rows] for at in basis_weighted[a]}, a, 0, lookups[a])
            for b in range(len(batches))
        ]
        stacked_steps.append(jnp.concatenate(parts, axis=0))
    stacked_u = [multiply(2.0 * stacked_steps[a], lpair[a]) for a in range(2)]

    def table_of(stacks, farthest):
        tables = []
        for a, stack in enumerate(stacks):
            table = {}
            for n, at in enumerate(order):
                if reach(a, at) > farthest:
                    continue
                first = (n // group) * rows + (n % group) * sc
                for m in range(sc):
                    value = None
                    for s in range(sc):
                        at_row = first + s * nrhs + (s - m) % sc
                        line = jnp.broadcast_to(stack[at_row : at_row + 1], (rows, width))
                        value = line if value is None else jnp.where(sub_row == s, line, value)
                    table[at, m] = value
            tables.append(table)
        return tables

    image_table = table_of([stacked[key(a, 0)] for a in range(2)], 1)
    step_table = table_of(stacked_steps, 2)
    u_table = table_of(stacked_u, 2)

    arrived(KROW)

    def widen(k):
        kt[k] = jnp.where(of_rhs, spread(kc[k]), 0.0)

    if ndev <= UNROLL:
        for k in range(ndev):
            widen(k)
    else:
        pl.loop(0, ndev)(widen)

    def pairwise(function, *operands):
        return [function(*(operand[a] for operand in operands)) for a in range(2)]

    image, step, lifted = advance(collect_tiles(0), True)
    turned, _, _ = collect_sums(0, False)
    residual = coarse(image, image_table, turned)
    precon = coarse(step, step_table, turned)
    u = coarse(lifted, u_table, turned)

    multipliers = [nothing, nothing]
    search = along = steps = lifts = gamma = step_size = None
    for iteration in range(ITERS):
        rd = iteration + 1
        last = rd == ITERS
        doubled = [2.0 * value for value in precon]
        dots = (residual[0] * precon[0] + residual[1] * precon[1], doubled[0] * u[0] + doubled[1] * u[1])
        publish(rd, doubled, u, dots)
        if iteration == 0:
            for what in arrivals:
                left(what)
        sent(rd - 1)
        if last:
            sent(rd)
        image, step, lifted = advance(collect_tiles(rd), not last)
        turned, gamma_new, curve = collect_sums(rd, True)
        image = coarse(image, image_table, turned)
        if not last:
            step = coarse(step, step_table, turned)
            lifted = coarse(lifted, u_table, turned)
        if iteration == 0:
            step_size = gamma_new / curve
            search, along, steps, lifts = precon, image, step, lifted
        else:
            ratio = gamma_new / gamma
            step_size = gamma_new / (curve - ratio * gamma_new / step_size)
            search = pairwise(lambda new, old: new + ratio * old, precon, search)
            along = pairwise(lambda new, old: new + ratio * old, image, along)
            if not last:
                steps = pairwise(lambda new, old: new + ratio * old, step, steps)
                lifts = pairwise(lambda new, old: new + ratio * old, lifted, lifts)
        gamma = gamma_new
        multipliers = pairwise(lambda value, move: value + step_size * move, multipliers, search)
        residual = pairwise(lambda value, move: value - step_size * move, residual, along)
        if not last:
            precon = pairwise(lambda value, move: value - step_size * move, precon, steps)
            u = pairwise(lambda value, move: value - step_size * move, u, lifts)
    first_row = jnp.full((rows, width), core, jnp.int32) == 0
    out[0] = pick(jnp.where(first_row, multipliers[0], multipliers[1]), backward)
    out[1] = pick(jnp.where(first_row, residual[0], residual[1]), backward)


def solution(mesh):
    nr, nc = mesh.shape["srow"], mesh.shape["scol"]
    slots = block_slots(nr // 2, nc)

    def body(loads, local_inverse, dirichlet, corner_coupling, coarse_inverse, partner):
        sr, sc, nrhs, width = loads.shape
        rows = sr * sc * nrhs
        ndev = nr * nc
        lanes = -(-(nrhs * nc * sc + 2 * nrhs) // 128) * 128
        dma = pltpu.SemaphoreType.DMA
        f32 = jnp.float32
        vmem = pl.BlockSpec(memory_space=pltpu.VMEM)
        hbm = pl.BlockSpec(memory_space=pl.ANY)
        rounds = ITERS + 1
        edge = width // 4
        out = pl.pallas_call(
            functools.partial(kernel, nr, nc, slots, sc, nrhs),
            out_shape=pltpu.VMEM((2, rows, width), f32),
            in_specs=[hbm] * 6,
            out_specs=vmem,
            scratch_shapes=[
                pltpu.VMEM((sc, coarse_inverse.shape[-1]), f32),
                pltpu.VMEM((rows, width), f32),
                pltpu.VMEM((sc, width), f32),
                pltpu.VMEM((sc, width), jnp.int32),
                pltpu.VMEM((2, sc, width, width), f32),
                pltpu.VMEM((2, sc, width, width), f32),
                pltpu.VMEM((2, sc * width, 2 * width), jnp.bfloat16),
                pltpu.VMEM((2, sc * width, 2 * width), jnp.bfloat16),
                pltpu.VMEM((2, sc * width, 2 * width), jnp.bfloat16),
                pltpu.VMEM((8, rows, width), f32),
                pltpu.VMEM((8, sc, width), f32),
                pltpu.VMEM((2 * len(slots), sc, width), f32),
                pltpu.VMEM((4, edge, width), f32),
                pltpu.VMEM((2, sc, edge, width), f32),
                pltpu.VMEM((ndev, sc, lanes), f32),
                pltpu.VMEM((ndev, rows, lanes), f32),
                pltpu.VMEM((rounds, len(slots), 2, rows, width), f32),
                pltpu.VMEM((rounds, ndev // 2, 2, lanes), f32),
                dma((6,)), dma((8,)), dma((8,)),
                dma((rounds,)), dma((rounds,)),
                dma((rounds,)), dma((rounds,)),
            ],
            compiler_params=pltpu.CompilerParams(collective_id=0, has_side_effects=True),
        )(
            loads.reshape(rows, width),
            corner_coupling.reshape(sc, width),
            coarse_inverse.reshape(sc, coarse_inverse.shape[-1]),
            partner.reshape(sc, width),
            local_inverse.reshape(sc, width, width),
            dirichlet.reshape(sc, width, width),
        )
        return out[0].reshape(loads.shape), out[1].reshape(loads.shape)

    whole, lists = P("srow", "scol", None, None), P("srow", "scol", None)
    return jax.shard_map(
        body,
        mesh=mesh,
        in_specs=(whole, whole, whole, lists, lists, lists),
        out_specs=(whole, whole),
        check_vma=False,
    )
```

```python
import functools

import jax
import jax.numpy as jnp
from jax import lax
from jax.experimental import pallas as pl
from jax.experimental.pallas import tpu as pltpu
from jax.sharding import PartitionSpec as P

ITERS = 3
MESH = pl.DeviceIdType.MESH
precise = lax.Precision.HIGHEST
UNROLL = 64
EAST, WEST, SOUTH, NORTH = 2, 4, 6, 7


def block_slots(nb, nc):
    slots = []
    for dp, dj in ((0, 0), (0, 1), (0, -1), (1, 1), (1, -1), (-1, 1), (-1, -1), (1, 0), (-1, 0)):
        off = (dp % nb, dj % nc)
        if off not in slots:
            slots.append(off)
    return slots


def kernel(nr, nc, slots, sc, nrhs, loads_in, cpl_in, cinv_in, part_in, linv, dirich, out,
           cinv, loads, cpl, part, lbuf, dbuf, lpair, dpair, fpair, loads_n, part_n, cpl_n, dside, dflat, kc, kt, ub, qb,
           local_sem, send_sem, recv_sem, u_send, u_recv, q_send, q_recv):
    rows, width = loads_n.shape[1:]
    edge = width // 4
    ndev = nr * nc
    nb = nr // 2
    nblocks = nb * nc
    ncols = nc * sc
    lanes = kt.shape[-1]
    i, j = lax.axis_index("srow"), lax.axis_index("scol")
    p, core = lax.div(i, 2), lax.rem(i, 2)
    near = [(0, 0), (1, 0), (0, 1), (1, 1), (0, nc - 1), (1, nc - 1), (nr - 1, 0), (2, 0)]
    LOADS, PART, CPL, LINV, DIRICH, SIDE, FLAT, KROW = range(8)

    def flip(index, mask):
        for bit in range(mask.bit_length()):
            if mask >> bit & 1:
                index = index + (1 << bit) - (2 << bit) * lax.rem(lax.div(index, 1 << bit), 2)
        return index

    powers = nb & (nb - 1) == 0 and nc & (nc - 1) == 0
    masks = sorted(((a, b) for a in range(nb) for b in range(nc) if a or b), key=lambda m: -(m[0] + m[1] // 2 + m[1] % 2))

    paired = ndev <= UNROLL and powers
    rows_to = [flip(i, 2 * a + c) for a in range(nb) for c in range(2)] if paired else []
    cols_to = [flip(j, b) for b in range(nc)] if paired else []

    def others(step):
        if paired:
            for a, b in [*masks, (0, 0)]:
                for c in range(2):
                    if a or b or c:
                        step(rows_to[2 * a + c], cols_to[b])
        elif ndev <= UNROLL:
            for k in range(1, ndev):
                step(lax.rem(i + k // nc, nr), lax.rem(j + k % nc, nc))
        else:
            @pl.loop(1, ndev)
            def _(k):
                step(lax.rem(i + lax.div(k, nc), nr), lax.rem(j + lax.rem(k, nc), nc))

    barrier = pltpu.get_barrier_semaphore()

    def greet(ti, tj):
        pl.semaphore_signal(barrier, inc=1, device_id=(ti, tj), device_id_type=MESH)

    fetches = [
        pltpu.make_async_copy(src, dst, local_sem.at[n])
        for n, (src, dst) in enumerate((
            (loads_in, loads), (part_in, part), (cpl_in, cpl), (cinv_in, cinv),
            (linv, lbuf.at[core]), (dirich, dbuf.at[core]),
        ))
    ]
    for fetch in fetches[:2]:
        fetch.start()
    others(greet)
    for fetch in fetches[2:]:
        fetch.start()

    row = lax.broadcasted_iota(jnp.int32, (rows, width), 0)
    lane = lax.broadcasted_iota(jnp.int32, (rows, width), 1)
    wrow = lax.broadcasted_iota(jnp.int32, (rows, lanes), 0)
    wlane = lax.broadcasted_iota(jnp.int32, (rows, lanes), 1)
    wrhs = lax.rem(wrow, nrhs)
    wsub = lax.div(wrow, nrhs)
    of_rhs = lax.div(wlane, ncols) == wrhs
    gamma_lane = wlane == nrhs * ncols + wrhs
    curve_lane = wlane == nrhs * ncols + nrhs + wrhs
    rhs_row = lax.rem(row, nrhs)
    sub_row = lax.div(row, nrhs)

    def spread(block):
        out = jnp.broadcast_to(block[0:1], (rows, block.shape[1]))
        which = lax.div(lax.broadcasted_iota(jnp.int32, out.shape, 0), nrhs)
        for s in range(1, sc):
            out = jnp.where(which == s, jnp.broadcast_to(block[s : s + 1], out.shape), out)
        return out

    def place(dj):
        column = lax.rem(j + dj, nc) * sc
        return wlane == wrhs * ncols + column + wsub

    def pick(values, index):
        return jnp.take_along_axis(values, index, axis=1, mode="promise_in_bounds")

    side = lax.div(lane, edge)
    half = lax.rem(side, 2)

    def odd(dr):
        return lax.rem(sub_row + dr, 2)

    def split(values):
        high = values.astype(jnp.bfloat16)
        return high, (values - high.astype(jnp.float32)).astype(jnp.bfloat16)

    def split_into(pair, blocks):
        for s, block in enumerate(blocks):
            high, low = split(block)
            pair[s * width : (s + 1) * width, 0:width] = high
            pair[s * width : (s + 1) * width, width : 2 * width] = low

    for fetch in fetches[:2]:
        fetch.wait()
    partner = spread(part[...])
    other = edge * (1 - 2 * half)
    mirrored = jnp.where((half == 1) & (partner >= 0), partner + side * edge, lane)
    crossed_over = jnp.where(half == 0, pltpu.roll(mirrored, width - edge, 1), pltpu.roll(mirrored, edge, 1))
    own_odd = odd(core)
    forward = jnp.where(own_odd == 1, crossed_over, mirrored)
    backward = jnp.where(own_odd == 1, mirrored + other, mirrored)
    loads_n[core] = pick(loads[...], forward)
    active_own = pick(jnp.where(partner >= 0, 1.0, 0.0), forward)
    for s in range(sc):
        part_n[core, s : s + 1] = active_own[s * nrhs : s * nrhs + 1]

    def reorder(buffer):
        for s in range(sc):
            index = jnp.broadcast_to(forward[s * nrhs : s * nrhs + 1], (width, width))
            buffer[core, s] = pick(pick(buffer[core, s], index).T, index)

    pl.semaphore_wait(barrier, ndev - 1)

    def push(src, dst, what, ti, tj):
        pltpu.make_async_remote_copy(
            src_ref=src, dst_ref=dst, send_sem=send_sem.at[what], recv_sem=recv_sem.at[what],
            device_id=(ti, tj), device_id_type=MESH).start()

    west_j, east_j = lax.rem(j + nc - 1, nc), lax.rem(j + 1, nc)
    beyond = lax.rem(p + 2 * core - 1 + nb, nb)
    partner_i = i + 1 - 2 * core
    around = [(EAST + core, 2 * p + t, west_j) for t in range(2)] + [(WEST + core, 2 * p + t, east_j) for t in range(2)]
    around += [(NORTH - core, 2 * beyond + t, j) for t in range(2)]
    toward = around + [(core, partner_i, j)]
    for n, ti, tj in toward:
        push(loads_n.at[core], loads_n.at[n], LOADS, ti, tj)
    for n, ti, tj in toward:
        push(part_n.at[core], part_n.at[n], PART, ti, tj)
    fetches[2].wait()
    coupling_own = pick(spread(cpl[...]), forward)
    for s in range(sc):
        cpl_n[core, s : s + 1] = coupling_own[s * nrhs : s * nrhs + 1]
    for n, (dp, dj) in enumerate(slots):
        for t in range(2):
            ti, tj = 2 * lax.rem(p - dp + nb, nb) + t, lax.rem(j - dj + nc, nc)
            if (dp, dj) == (0, 0):
                if t == 0:
                    push(cpl_n.at[core], cpl_n.at[core], CPL, partner_i, j)
            else:
                push(cpl_n.at[core], cpl_n.at[2 * n + core], CPL, ti, tj)
    tile_lane = lax.broadcasted_iota(jnp.int32, (ncols, lanes), 1)
    tile_row = lax.broadcasted_iota(jnp.int32, (ncols, lanes), 0)
    tiler = jnp.where(lax.rem(tile_lane, ncols) == tile_row, 1.0, 0.0)
    fetches[3].wait()
    tiled = jnp.dot(spread(cinv[...]), tiler, precision=precise, preferred_element_type=jnp.float32)
    for s in range(sc):
        kc[core * nc, s : s + 1] = tiled[s * nrhs : s * nrhs + 1]
    own_place = place(0)
    def send_k(ti, tj):
        slot = lax.rem(i - 2 * lax.div(ti, 2) + nr, nr) * nc + lax.rem(j - tj + nc, nc)
        push(kc.at[core * nc], kc.at[slot], KROW, ti, tj)

    others(send_k)
    fetches[4].wait()
    reorder(lbuf)
    push(lbuf.at[core], lbuf.at[core], LINV, partner_i, j)
    fetches[5].wait()
    reorder(dbuf)

    def facing_rows(s, group):
        return dbuf.at[core, s, pl.ds(pl.multiple_of(group * edge, edge), edge)]

    for n, ti, tj in around[:2]:
        push(facing_rows(0, lax.rem(core, 2)), dside.at[core], SIDE, ti, tj)
    for n, ti, tj in around[2:4]:
        push(facing_rows(sc - 1, 1 - lax.rem(core + sc - 1, 2)), dside.at[2 + core], SIDE, ti, tj)
    for n, ti, tj in around[4:]:
        for s in range(sc):
            push(facing_rows(s, 2 + s % 2), dflat.at[1 - core, s], FLAT, ti, tj)
    push(dbuf.at[core], dbuf.at[core], DIRICH, partner_i, j)

    arrivals = {
        LOADS: loads_n.at[pl.ds(0, 7)], PART: part_n.at[pl.ds(0, 7)], CPL: cpl_n.at[pl.ds(0, 2 * len(slots) - 1)],
        LINV: lbuf.at[0], DIRICH: dbuf.at[0], SIDE: dside, FLAT: dflat, KROW: kc.at[pl.ds(0, ndev - 1)],
    }

    def arrived(what):
        pltpu.make_async_copy(arrivals[what], arrivals[what], recv_sem.at[what]).wait()

    def left(what):
        pltpu.make_async_copy(arrivals[what], arrivals[what], send_sem.at[what]).wait()

    def meet(mine, before, after, south, north, dr, active):
        if rows == 2 * nrhs:
            lateral = pltpu.roll(jnp.where(half == odd(dr + 1), before, after), nrhs, 0)
        else:
            lateral = jnp.where(half == odd(dr), pltpu.roll(before, nrhs, 0), pltpu.roll(after, rows - nrhs, 0))
        facing = jnp.where(side < 2, lateral, jnp.where(half == odd(dr), south, north))
        return jnp.where(active, mine - facing, 0.0)

    def jump(mine, west_tile, east_tile, south, north, dr, active):
        before = jnp.where(row < rows - nrhs, mine, west_tile)
        after = jnp.where(row < nrhs, east_tile, mine)
        return meet(mine, before, after, south, north, dr, active)

    def key(dr, dj):
        return (dr % nr, dj % nc)

    def jump_at(tiles, dr, dj, lookup):
        mine = tiles[key(dr, dj)]
        beyond = [tiles.get(key(*at), mine) for at in ((dr, dj - 1), (dr, dj + 1), (dr - 1, dj), (dr + 1, dj))]
        return jump(mine, *beyond, dr, lookup)

    def multiply(values, pair):
        total = values.shape[0]
        high = values.astype(jnp.bfloat16).astype(jnp.float32)
        stacked = jnp.concatenate([high, values - high], axis=0)
        sub = lax.rem(lax.div(lax.broadcasted_iota(jnp.int32, stacked.shape, 0), nrhs), sc)
        wide = jnp.concatenate([jnp.where(sub == s, stacked, 0.0) for s in range(sc)], axis=1)
        product = jnp.dot(wide.astype(jnp.bfloat16), pair, preferred_element_type=jnp.float32)
        return (product[0:total, 0:width] + product[total:, 0:width]) + (product[0:total, width:] + product[total:, width:])

    def lane_sum(values):
        return jnp.sum(values, axis=1, keepdims=True)

    keys = {key(2 * dp + a, dj): (n, a) for n, (dp, dj) in enumerate(slots) for a in range(2)}

    def reach(a, at):
        return min((at[0] - a) % nr, (a - at[0]) % nr) + min(at[1], nc - at[1])

    def q_target(tp, tj):
        return lax.rem(p - tp + nb, nb) * nc + lax.rem(j - tj + nc, nc), 2 * tp + 1 - core, tj

    q_targets = []
    if nblocks <= UNROLL:
        for a, b in masks:
            q_targets.append(q_target(flip(p, a), flip(j, b)) if powers else q_target(lax.rem(p + a, nb), lax.rem(j + b, nc)))
    u_targets = [
        (n, 2 * lax.rem(p - dp + nb, nb) + 1 - core, lax.rem(j - dj + nc, nc)) for n, (dp, dj) in enumerate(slots) if n
    ]
    u_targets.sort(key=lambda target: (slots[target[0]][1] == 0, slots[target[0]][0] == 0))

    def publish(rd, values, u, dots):
        for a in range(2):
            ub[rd, 0, a] = u[a]

        def across(src, dst, send, recv, ti, tj):
            pltpu.make_async_remote_copy(
                src_ref=src, dst_ref=dst, send_sem=send.at[rd], recv_sem=recv.at[rd],
                device_id=(ti, tj), device_id_type=MESH).start()

        for n, ti, tj in u_targets:
            across(ub.at[rd, 0], ub.at[rd, n], u_send, u_recv, ti, tj)
        for a in range(2):
            message = jnp.where(own_place, lane_sum(couplings[a, 0] * values[a]), 0.0)
            if dots is not None and a == 0:
                gamma, curve = dots
                message = jnp.where(gamma_lane, lane_sum(gamma), message)
                message = jnp.where(curve_lane, lane_sum(curve), message)
            qb[rd, 0, a : a + 1] = jnp.sum(message, axis=0, keepdims=True)
        if nblocks <= UNROLL:
            for slot, ti, tj in q_targets:
                across(qb.at[rd, 0], qb.at[rd, slot], q_send, q_recv, ti, tj)
        else:
            @pl.loop(1, nblocks)
            def _(k):
                slot, ti, tj = q_target(lax.rem(p + lax.div(k, nc), nb), lax.rem(j + lax.rem(k, nc), nc))
                across(qb.at[rd, 0], qb.at[rd, slot], q_send, q_recv, ti, tj)

    def sent(rd):
        bytes_q = qb.at[rd, pl.ds(1, nblocks - 1)]
        pltpu.make_async_copy(bytes_q, bytes_q, q_send.at[rd]).wait()
        bytes_u = ub.at[rd, pl.ds(1, len(slots) - 1)]
        pltpu.make_async_copy(bytes_u, bytes_u, u_send.at[rd]).wait()

    def collect_tiles(rd):
        bytes_u = ub.at[rd, pl.ds(1, len(slots) - 1)]
        pltpu.make_async_copy(bytes_u, bytes_u, u_recv.at[rd]).wait()
        return {at: ub[rd, n, a] for at, (n, a) in keys.items()}

    def collect_sums(rd, want_dots):
        bytes_q = qb.at[rd, pl.ds(1, nblocks - 1)]
        pltpu.make_async_copy(bytes_q, bytes_q, q_recv.at[rd]).wait()
        sums = [jnp.sum(qb[rd, pl.ds(d * nc, nc)], axis=0) for d in range(nb)]
        band = [jnp.broadcast_to(sums[d // 2][d % 2 : d % 2 + 1], (rows, lanes)) for d in range(nr)]
        cols = {}

        def column(k, d):
            return lane_sum(band[d] * kt[k])

        gamma = curve = None
        if want_dots:
            cross = jnp.zeros((rows, lanes), jnp.float32)
            for d in range(nr):
                total = jnp.zeros((rows, lanes), jnp.float32)
                if ndev <= UNROLL:
                    for e in range(nc):
                        cols[(d, e)] = column(d * nc + e, d)
                        total = total + jnp.where(place(e), cols[(d, e)], 0.0)
                else:
                    def add(e, total):
                        return total + jnp.where(place(e), column(d * nc + e, d), 0.0)
                    total = lax.fori_loop(0, nc, add, total)
                cross = cross + total * band[d]
            everything = functools.reduce(jnp.add, band)
            crossed = jnp.broadcast_to(jnp.sum(cross, axis=0, keepdims=True), (rows, lanes))
            curve = lane_sum(jnp.where(of_rhs, crossed, 0.0) + jnp.where(curve_lane, everything, 0.0))
            gamma = lane_sum(jnp.where(gamma_lane, everything, 0.0))
        turned = {}
        for at in keys:
            if at not in cols:
                cols[at] = column(at[0] * nc + at[1], at[0])
            wide_col = jnp.broadcast_to(cols[at], (rows, width))
            for m in range(sc):
                turned[at, m] = pltpu.roll(wide_col, m * nrhs, 0) if m else wide_col
        return turned, gamma, curve

    def beside(a):
        return [key(a, 1), key(2, 0) if a else key(-1, 0)]

    def precondition(images):
        weighted = []
        for a in range(2):
            total = images[key(a, 0)].shape[0]
            ring = multiply(jnp.concatenate([images[at] for at in beside(a)], axis=0), fpair[a])
            weighted.append({at: ring[m * total : (m + 1) * total] for m, at in enumerate(beside(a))})
            weighted[a][key(a, -1)] = weighted[a][key(a, 1)]
        for a in range(2):
            mine = multiply(images[key(a, 0)], dpair[a])
            for ring in weighted:
                ring[key(a, 0)] = mine
        return weighted

    def jump_sides(tiles, a):
        east, mine, west = (tiles[key(a, dj)] for dj in (1, 0, -1))
        before = jnp.where(row < rows - nrhs, west, mine)
        after = jnp.where(row < nrhs, mine, east)
        flat = [jnp.where(row < nrhs, tiles.get(key(a + d, 1), east), tiles.get(key(a + d, -1), west)) for d in (-1, 1)]
        return meet(jnp.where(row < nrhs, east, west), before, after, *flat, a, side_lookups[a])

    def images_of(tiles):
        images = {key(*near[n]): jump_at(tiles, *near[n], lookups[n]) for n in (0, 1, SOUTH, NORTH)}
        for a in range(2):
            images[key(a, 1)] = jump_sides(tiles, a)
        return images

    def advance(tiles, keep):
        if not keep:
            return [jump_at(tiles, a, 0, lookups[a]) for a in range(2)], None
        images = images_of(tiles)
        weighted = precondition(images)
        step = [jump_at(weighted[a], a, 0, lookups[a]) for a in range(2)]
        return [images[key(a, 0)] for a in range(2)], step

    def lift(step):
        return [multiply(step[a], lpair[a]) for a in range(2)]

    def coarse(table, turned):
        sums = []
        for a in range(2):
            terms = [table[a][at, m] * turned[at, m] for at, m in table[a]]
            while len(terms) > 1:
                terms = [sum(terms[k + 1 : k + 2], terms[k]) for k in range(0, len(terms), 2)]
            sums.append(terms[0])
        return sums

    arrived(LINV)
    for a in range(2):
        split_into(lpair.at[a], [2.0 * lbuf[a, s] for s in range(sc)])
        fpair[a] = jnp.zeros(fpair.shape[1:], jnp.bfloat16)

    arrived(PART)
    partners = [spread(part_n[n]) for n in range(len(near))]
    lookups = [partner > 0.5 for partner in partners]
    side_lookups = [jnp.where(row < nrhs, partners[EAST + a], partners[WEST + a]) > 0.5 for a in range(2)]
    arrived(CPL)
    couplings = {at: spread(cpl_n[2 * n + a]) for at, (n, a) in keys.items()}
    arrived(LOADS)
    load_tiles = {key(*at): loads_n[n] for n, at in enumerate(near)}
    start = [jump_at(load_tiles, a, 0, lookups[a]) for a in range(2)]
    publish(0, start, [multiply(0.5 * start[a], lpair[a]) for a in range(2)], None)

    arrived(SIDE)
    arrived(FLAT)
    arrived(DIRICH)

    def edge_into(block, a, s, first):
        high, low = split(2.0 * block.T)
        fpair[a, s * width : (s + 1) * width, first : first + edge] = high
        fpair[a, s * width : (s + 1) * width, width + first : width + first + edge] = low

    for a in range(2):
        split_into(dpair.at[a], [2.0 * dbuf[a, s] for s in range(sc)])
        edge_into(dside[a], a, 0, edge * (1 - (a + sc - 1) % 2))
        edge_into(dside[2 + a], a, sc - 1, edge * (a % 2))
        for s in range(sc):
            edge_into(dflat[a, s], a, s, edge * (2 + s % 2))

    group = nrhs // sc
    order = list(keys)
    nothing = jnp.zeros((rows, width), jnp.float32)
    batches = [order[first : first + group] for first in range(0, len(order), group)]
    basis_images = []
    for batch in batches:
        tiles = {at: nothing for at in order}
        for g, at in enumerate(batch):
            tiles[at] = jnp.where(rhs_row == g * sc + sub_row, couplings[at], 0.0)
        basis_images.append(images_of(tiles))
    stacked = {at: jnp.concatenate([images[at] for images in basis_images], axis=0) for at in basis_images[0]}
    basis_weighted = precondition(stacked)
    stacked_steps = []
    for a in range(2):
        parts = [
            jump_at({at: basis_weighted[a][at][b * rows : (b + 1) * rows] for at in basis_weighted[a]}, a, 0, lookups[a])
            for b in range(len(batches))
        ]
        stacked_steps.append(jnp.concatenate(parts, axis=0))
    stacked_u = [multiply(stacked_steps[a], lpair[a]) for a in range(2)]

    def table_of(stacks, farthest):
        tables = []
        for a, stack in enumerate(stacks):
            table = {}
            for n, at in enumerate(order):
                if reach(a, at) > farthest:
                    continue
                first = (n // group) * rows + (n % group) * sc
                for m in range(sc):
                    value = None
                    for s in range(sc):
                        at_row = first + s * nrhs + (s - m) % sc
                        line = jnp.broadcast_to(stack[at_row : at_row + 1], (rows, width))
                        value = line if value is None else jnp.where(sub_row == s, line, value)
                    table[at, m] = value
            tables.append(table)
        return tables

    image_table = table_of([stacked[key(a, 0)] for a in range(2)], 1)
    step_table = table_of(stacked_steps, 2)
    u_table = table_of(stacked_u, 2)

    arrived(KROW)

    def widen(k):
        kt[k] = jnp.where(of_rhs, spread(kc[k]), 0.0)

    if ndev <= UNROLL:
        for k in range(ndev):
            widen(k)
    else:
        pl.loop(0, ndev)(widen)

    def pairwise(function, *operands):
        return [function(*(operand[a] for operand in operands)) for a in range(2)]

    def plus(left, right):
        return pairwise(jnp.add, left, right)

    image, step = advance(collect_tiles(0), True)
    turned, _, _ = collect_sums(0, False)
    lifted = lift(step)
    residual = plus(image, coarse(image_table, turned))
    precon = plus(step, coarse(step_table, turned))
    u = plus(lifted, coarse(u_table, turned))

    multipliers = [nothing, nothing]
    search = along = steps = lifts = gamma = step_size = ratio = None
    for iteration in range(ITERS):
        rd = iteration + 1
        last = rd == ITERS
        doubled = [2.0 * value for value in precon]
        dots = (residual[0] * precon[0] + residual[1] * precon[1], doubled[0] * u[0] + doubled[1] * u[1])
        publish(rd, doubled, u, dots)
        if iteration == 0:
            for what in arrivals:
                left(what)
        sent(rd - 1)
        if last:
            sent(rd)
        image, step = advance(collect_tiles(rd), not last)
        turned, gamma_new, curve = collect_sums(rd, True)
        if iteration == 0:
            step_size = gamma_new / curve
            search = precon
        else:
            ratio = gamma_new / gamma
            step_size = gamma_new / (curve - ratio * gamma_new / step_size)
            search = pairwise(lambda new, old: new + ratio * old, precon, search)

        def known(table, old):
            fixed = coarse(table, turned)
            return fixed if old is None else pairwise(lambda new, before: new + ratio * before, fixed, old)

        def descend(value, fixed, new):
            return pairwise(lambda v, f, n: (v - step_size * f) - step_size * n, value, fixed, new)

        gamma = gamma_new
        multipliers = pairwise(lambda value, move: value + step_size * move, multipliers, search)
        fixed = known(image_table, along)
        residual = descend(residual, fixed, image)
        along = plus(image, fixed)
        if not last:
            fixed = known(step_table, steps)
            precon = descend(precon, fixed, step)
            steps = plus(step, fixed)
            fixed = known(u_table, lifts)
            lifted = lift(step)
            u = descend(u, fixed, lifted)
            lifts = plus(lifted, fixed)
    first_row = jnp.full((rows, width), core, jnp.int32) == 0
    out[0] = pick(jnp.where(first_row, multipliers[0], multipliers[1]), backward)
    out[1] = pick(jnp.where(first_row, residual[0], residual[1]), backward)


def solution(mesh):
    nr, nc = mesh.shape["srow"], mesh.shape["scol"]
    slots = block_slots(nr // 2, nc)

    def body(loads, local_inverse, dirichlet, corner_coupling, coarse_inverse, partner):
        sr, sc, nrhs, width = loads.shape
        rows = sr * sc * nrhs
        ndev = nr * nc
        lanes = -(-(nrhs * nc * sc + 2 * nrhs) // 128) * 128
        dma = pltpu.SemaphoreType.DMA
        f32 = jnp.float32
        vmem = pl.BlockSpec(memory_space=pltpu.VMEM)
        hbm = pl.BlockSpec(memory_space=pl.ANY)
        rounds = ITERS + 1
        edge = width // 4
        out = pl.pallas_call(
            functools.partial(kernel, nr, nc, slots, sc, nrhs),
            out_shape=pltpu.VMEM((2, rows, width), f32),
            in_specs=[hbm] * 6,
            out_specs=vmem,
            scratch_shapes=[
                pltpu.VMEM((sc, coarse_inverse.shape[-1]), f32),
                pltpu.VMEM((rows, width), f32),
                pltpu.VMEM((sc, width), f32),
                pltpu.VMEM((sc, width), jnp.int32),
                pltpu.VMEM((2, sc, width, width), f32),
                pltpu.VMEM((2, sc, width, width), f32),
                pltpu.VMEM((2, sc * width, 2 * width), jnp.bfloat16),
                pltpu.VMEM((2, sc * width, 2 * width), jnp.bfloat16),
                pltpu.VMEM((2, sc * width, 2 * width), jnp.bfloat16),
                pltpu.VMEM((8, rows, width), f32),
                pltpu.VMEM((8, sc, width), f32),
                pltpu.VMEM((2 * len(slots), sc, width), f32),
                pltpu.VMEM((4, edge, width), f32),
                pltpu.VMEM((2, sc, edge, width), f32),
                pltpu.VMEM((ndev, sc, lanes), f32),
                pltpu.VMEM((ndev, rows, lanes), f32),
                pltpu.VMEM((rounds, len(slots), 2, rows, width), f32),
                pltpu.VMEM((rounds, ndev // 2, 2, lanes), f32),
                dma((6,)), dma((8,)), dma((8,)),
                dma((rounds,)), dma((rounds,)),
                dma((rounds,)), dma((rounds,)),
            ],
            compiler_params=pltpu.CompilerParams(collective_id=0, has_side_effects=True),
        )(
            loads.reshape(rows, width),
            corner_coupling.reshape(sc, width),
            coarse_inverse.reshape(sc, coarse_inverse.shape[-1]),
            partner.reshape(sc, width),
            local_inverse.reshape(sc, width, width),
            dirichlet.reshape(sc, width, width),
        )
        return out[0].reshape(loads.shape), out[1].reshape(loads.shape)

    whole, lists = P("srow", "scol", None, None), P("srow", "scol", None)
    return jax.shard_map(
        body,
        mesh=mesh,
        in_specs=(whole, whole, whole, lists, lists, lists),
        out_specs=(whole, whole),
        check_vma=False,
    )
```

```python
import functools

import jax
import jax.numpy as jnp
from jax import lax
from jax.experimental import pallas as pl
from jax.experimental.pallas import tpu as pltpu
from jax.sharding import PartitionSpec as P

ITERS = 3
MESH = pl.DeviceIdType.MESH
precise = lax.Precision.HIGHEST
UNROLL = 64
EAST, WEST, SOUTH, NORTH = 2, 4, 6, 7


def block_slots(nb, nc):
    slots = []
    for dp, dj in ((0, 0), (0, 1), (0, -1), (1, 1), (1, -1), (-1, 1), (-1, -1), (1, 0), (-1, 0)):
        off = (dp % nb, dj % nc)
        if off not in slots:
            slots.append(off)
    return slots


def kernel(nr, nc, slots, sc, nrhs, loads_in, cpl_in, cinv_in, part_in, linv, dirich, out,
           cinv, loads, cpl, part, lbuf, dbuf, lpair, dpair, fpair, loads_n, part_n, cpl_n, dside, dflat, kc, kt, ub, qb,
           local_sem, send_sem, recv_sem, u_send, u_recv, q_send, q_recv):
    rows, width = loads_n.shape[1:]
    edge = width // 4
    ndev = nr * nc
    nb = nr // 2
    nblocks = nb * nc
    ncols = nc * sc
    lanes = kt.shape[-1]
    i, j = lax.axis_index("srow"), lax.axis_index("scol")
    p, core = lax.div(i, 2), lax.rem(i, 2)
    near = [(0, 0), (1, 0), (0, 1), (1, 1), (0, nc - 1), (1, nc - 1), (nr - 1, 0), (2, 0)]
    LOADS, PART, CPL, LINV, DIRICH, SIDE, FLAT, KROW, PAIR_PART, PAIR_CPL = range(10)

    def flip(index, mask):
        for bit in range(mask.bit_length()):
            if mask >> bit & 1:
                index = index + (1 << bit) - (2 << bit) * lax.rem(lax.div(index, 1 << bit), 2)
        return index

    powers = nb & (nb - 1) == 0 and nc & (nc - 1) == 0
    masks = sorted(((a, b) for a in range(nb) for b in range(nc) if a or b), key=lambda m: -(m[0] + m[1] // 2 + m[1] % 2))

    paired = ndev <= UNROLL and powers
    rows_to = [flip(i, 2 * a + c) for a in range(nb) for c in range(2)] if paired else []
    cols_to = [flip(j, b) for b in range(nc)] if paired else []

    def others(step):
        if paired:
            for a, b in [*masks, (0, 0)]:
                for c in range(2):
                    if a or b or c:
                        step(rows_to[2 * a + c], cols_to[b])
        elif ndev <= UNROLL:
            for k in range(1, ndev):
                step(lax.rem(i + k // nc, nr), lax.rem(j + k % nc, nc))
        else:
            @pl.loop(1, ndev)
            def _(k):
                step(lax.rem(i + lax.div(k, nc), nr), lax.rem(j + lax.rem(k, nc), nc))

    barrier = pltpu.get_barrier_semaphore()

    def greet(ti, tj):
        pl.semaphore_signal(barrier, inc=1, device_id=(ti, tj), device_id_type=MESH)

    fetches = [
        pltpu.make_async_copy(src, dst, local_sem.at[n])
        for n, (src, dst) in enumerate((
            (loads_in, loads), (part_in, part), (cpl_in, cpl), (cinv_in, cinv),
            (linv, lbuf.at[core]), (dirich, dbuf.at[core]),
        ))
    ]
    for fetch in fetches[:2]:
        fetch.start()
    others(greet)
    for fetch in fetches[2:]:
        fetch.start()

    row = lax.broadcasted_iota(jnp.int32, (rows, width), 0)
    lane = lax.broadcasted_iota(jnp.int32, (rows, width), 1)
    wrow = lax.broadcasted_iota(jnp.int32, (rows, lanes), 0)
    wlane = lax.broadcasted_iota(jnp.int32, (rows, lanes), 1)
    wrhs = lax.rem(wrow, nrhs)
    wsub = lax.div(wrow, nrhs)
    of_rhs = lax.div(wlane, ncols) == wrhs
    gamma_lane = wlane == nrhs * ncols + wrhs
    curve_lane = wlane == nrhs * ncols + nrhs + wrhs
    rhs_row = lax.rem(row, nrhs)
    sub_row = lax.div(row, nrhs)

    def spread(block):
        out = jnp.broadcast_to(block[0:1], (rows, block.shape[1]))
        which = lax.div(lax.broadcasted_iota(jnp.int32, out.shape, 0), nrhs)
        for s in range(1, sc):
            out = jnp.where(which == s, jnp.broadcast_to(block[s : s + 1], out.shape), out)
        return out

    def place(dj):
        column = lax.rem(j + dj, nc) * sc
        return wlane == wrhs * ncols + column + wsub

    def pick(values, index):
        return jnp.take_along_axis(values, index, axis=1, mode="promise_in_bounds")

    side = lax.div(lane, edge)
    half = lax.rem(side, 2)

    def odd(dr):
        return lax.rem(sub_row + dr, 2)

    def split(values):
        high = values.astype(jnp.bfloat16)
        return high, (values - high.astype(jnp.float32)).astype(jnp.bfloat16)

    def split_into(pair, blocks):
        for s, block in enumerate(blocks):
            high, low = split(block)
            pair[s * width : (s + 1) * width, 0:width] = high
            pair[s * width : (s + 1) * width, width : 2 * width] = low

    for fetch in fetches[:2]:
        fetch.wait()
    partner = spread(part[...])
    other = edge * (1 - 2 * half)
    mirrored = jnp.where((half == 1) & (partner >= 0), partner + side * edge, lane)
    crossed_over = jnp.where(half == 0, pltpu.roll(mirrored, width - edge, 1), pltpu.roll(mirrored, edge, 1))
    own_odd = odd(core)
    forward = jnp.where(own_odd == 1, crossed_over, mirrored)
    backward = jnp.where(own_odd == 1, mirrored + other, mirrored)
    loads_n[core] = pick(loads[...], forward)
    active_own = pick(jnp.where(partner >= 0, 1.0, 0.0), forward)
    for s in range(sc):
        part_n[core, s : s + 1] = active_own[s * nrhs : s * nrhs + 1]

    def reorder(buffer):
        for s in range(sc):
            index = jnp.broadcast_to(forward[s * nrhs : s * nrhs + 1], (width, width))
            buffer[core, s] = pick(pick(buffer[core, s], index).T, index)

    pl.semaphore_wait(barrier, ndev - 1)

    def push(src, dst, what, ti, tj):
        pltpu.make_async_remote_copy(
            src_ref=src, dst_ref=dst, send_sem=send_sem.at[what], recv_sem=recv_sem.at[what],
            device_id=(ti, tj), device_id_type=MESH).start()

    west_j, east_j = lax.rem(j + nc - 1, nc), lax.rem(j + 1, nc)
    beyond = lax.rem(p + 2 * core - 1 + nb, nb)
    partner_i = i + 1 - 2 * core
    around = [(EAST + core, 2 * p + t, west_j) for t in range(2)] + [(WEST + core, 2 * p + t, east_j) for t in range(2)]
    around += [(NORTH - core, 2 * beyond + t, j) for t in range(2)]
    toward = around + [(core, partner_i, j)]
    for n, ti, tj in toward:
        push(loads_n.at[core], loads_n.at[n], LOADS, ti, tj)
    push(part_n.at[core], part_n.at[core], PAIR_PART, partner_i, j)
    for n, ti, tj in around:
        push(part_n.at[core], part_n.at[n], PART, ti, tj)
    fetches[2].wait()
    coupling_own = pick(spread(cpl[...]), forward)
    for s in range(sc):
        cpl_n[core, s : s + 1] = coupling_own[s * nrhs : s * nrhs + 1]
    push(cpl_n.at[core], cpl_n.at[core], PAIR_CPL, partner_i, j)
    for n, (dp, dj) in enumerate(slots):
        for t in range(2):
            ti, tj = 2 * lax.rem(p - dp + nb, nb) + t, lax.rem(j - dj + nc, nc)
            if n:
                push(cpl_n.at[core], cpl_n.at[2 * n + core], CPL, ti, tj)
    tile_lane = lax.broadcasted_iota(jnp.int32, (ncols, lanes), 1)
    tile_row = lax.broadcasted_iota(jnp.int32, (ncols, lanes), 0)
    tiler = jnp.where(lax.rem(tile_lane, ncols) == tile_row, 1.0, 0.0)
    fetches[3].wait()
    tiled = jnp.dot(spread(cinv[...]), tiler, precision=precise, preferred_element_type=jnp.float32)
    for s in range(sc):
        kc[core * nc, s : s + 1] = tiled[s * nrhs : s * nrhs + 1]
    own_place = place(0)
    def send_k(ti, tj):
        slot = lax.rem(i - 2 * lax.div(ti, 2) + nr, nr) * nc + lax.rem(j - tj + nc, nc)
        push(kc.at[core * nc], kc.at[slot], KROW, ti, tj)

    others(send_k)
    fetches[4].wait()
    reorder(lbuf)
    push(lbuf.at[core], lbuf.at[core], LINV, partner_i, j)
    fetches[5].wait()
    reorder(dbuf)

    def facing_rows(s, group):
        return dbuf.at[core, s, pl.ds(pl.multiple_of(group * edge, edge), edge)]

    for n, ti, tj in around[:2]:
        push(facing_rows(0, lax.rem(core, 2)), dside.at[core], SIDE, ti, tj)
    for n, ti, tj in around[2:4]:
        push(facing_rows(sc - 1, 1 - lax.rem(core + sc - 1, 2)), dside.at[2 + core], SIDE, ti, tj)
    for n, ti, tj in around[4:]:
        for s in range(sc):
            push(facing_rows(s, 2 + s % 2), dflat.at[1 - core, s], FLAT, ti, tj)
    push(dbuf.at[core], dbuf.at[core], DIRICH, partner_i, j)

    arrivals = {
        LOADS: loads_n.at[pl.ds(0, 7)], PART: part_n.at[pl.ds(0, 6)], CPL: cpl_n.at[pl.ds(0, 2 * len(slots) - 2)],
        PAIR_PART: part_n.at[0], PAIR_CPL: cpl_n.at[0],
        LINV: lbuf.at[0], DIRICH: dbuf.at[0], SIDE: dside, FLAT: dflat, KROW: kc.at[pl.ds(0, ndev - 1)],
    }

    def arrived(what):
        pltpu.make_async_copy(arrivals[what], arrivals[what], recv_sem.at[what]).wait()

    def left(what):
        pltpu.make_async_copy(arrivals[what], arrivals[what], send_sem.at[what]).wait()

    def meet(mine, before, after, south, north, dr, active):
        if rows == 2 * nrhs:
            lateral = pltpu.roll(jnp.where(half == odd(dr + 1), before, after), nrhs, 0)
        else:
            lateral = jnp.where(half == odd(dr), pltpu.roll(before, nrhs, 0), pltpu.roll(after, rows - nrhs, 0))
        facing = jnp.where(side < 2, lateral, jnp.where(half == odd(dr), south, north))
        return jnp.where(active, mine - facing, 0.0)

    def jump(mine, west_tile, east_tile, south, north, dr, active):
        before = jnp.where(row < rows - nrhs, mine, west_tile)
        after = jnp.where(row < nrhs, east_tile, mine)
        return meet(mine, before, after, south, north, dr, active)

    def key(dr, dj):
        return (dr % nr, dj % nc)

    def jump_at(tiles, dr, dj, lookup):
        mine = tiles[key(dr, dj)]
        beyond = [tiles.get(key(*at), mine) for at in ((dr, dj - 1), (dr, dj + 1), (dr - 1, dj), (dr + 1, dj))]
        return jump(mine, *beyond, dr, lookup)

    def multiply(values, pair):
        total = values.shape[0]
        high = values.astype(jnp.bfloat16).astype(jnp.float32)
        stacked = jnp.concatenate([high, values - high], axis=0)
        sub = lax.rem(lax.div(lax.broadcasted_iota(jnp.int32, stacked.shape, 0), nrhs), sc)
        wide = jnp.concatenate([jnp.where(sub == s, stacked, 0.0) for s in range(sc)], axis=1)
        product = jnp.dot(wide.astype(jnp.bfloat16), pair, preferred_element_type=jnp.float32)
        return (product[0:total, 0:width] + product[total:, 0:width]) + (product[0:total, width:] + product[total:, width:])

    def lane_sum(values):
        return jnp.sum(values, axis=1, keepdims=True)

    keys = {key(2 * dp + a, dj): (n, a) for n, (dp, dj) in enumerate(slots) for a in range(2)}

    def reach(a, at):
        return min((at[0] - a) % nr, (a - at[0]) % nr) + min(at[1], nc - at[1])

    def q_target(tp, tj):
        return lax.rem(p - tp + nb, nb) * nc + lax.rem(j - tj + nc, nc), 2 * tp + 1 - core, tj

    q_targets = []
    if nblocks <= UNROLL:
        for a, b in masks:
            q_targets.append(q_target(flip(p, a), flip(j, b)) if powers else q_target(lax.rem(p + a, nb), lax.rem(j + b, nc)))
    u_targets = [
        (n, 2 * lax.rem(p - dp + nb, nb) + 1 - core, lax.rem(j - dj + nc, nc)) for n, (dp, dj) in enumerate(slots) if n
    ]
    u_targets.sort(key=lambda target: (slots[target[0]][1] == 0, slots[target[0]][0] == 0))

    def publish(rd, values, u, dots):
        for a in range(2):
            ub[rd, 0, a] = u[a]

        def across(src, dst, send, recv, ti, tj):
            pltpu.make_async_remote_copy(
                src_ref=src, dst_ref=dst, send_sem=send.at[rd], recv_sem=recv.at[rd],
                device_id=(ti, tj), device_id_type=MESH).start()

        for n, ti, tj in u_targets:
            across(ub.at[rd, 0], ub.at[rd, n], u_send, u_recv, ti, tj)
        for a in range(2):
            message = jnp.where(own_place, lane_sum(couplings[a, 0] * values[a]), 0.0)
            if dots is not None and a == 0:
                gamma, curve = dots
                message = jnp.where(gamma_lane, lane_sum(gamma), message)
                message = jnp.where(curve_lane, lane_sum(curve), message)
            qb[rd, 0, a : a + 1] = jnp.sum(message, axis=0, keepdims=True)
        if nblocks <= UNROLL:
            for slot, ti, tj in q_targets:
                across(qb.at[rd, 0], qb.at[rd, slot], q_send, q_recv, ti, tj)
        else:
            @pl.loop(1, nblocks)
            def _(k):
                slot, ti, tj = q_target(lax.rem(p + lax.div(k, nc), nb), lax.rem(j + lax.rem(k, nc), nc))
                across(qb.at[rd, 0], qb.at[rd, slot], q_send, q_recv, ti, tj)

    def sent(rd):
        bytes_q = qb.at[rd, pl.ds(1, nblocks - 1)]
        pltpu.make_async_copy(bytes_q, bytes_q, q_send.at[rd]).wait()
        bytes_u = ub.at[rd, pl.ds(1, len(slots) - 1)]
        pltpu.make_async_copy(bytes_u, bytes_u, u_send.at[rd]).wait()

    def collect_tiles(rd):
        bytes_u = ub.at[rd, pl.ds(1, len(slots) - 1)]
        pltpu.make_async_copy(bytes_u, bytes_u, u_recv.at[rd]).wait()
        return {at: ub[rd, n, a] for at, (n, a) in keys.items()}

    def collect_sums(rd, want_dots):
        bytes_q = qb.at[rd, pl.ds(1, nblocks - 1)]
        pltpu.make_async_copy(bytes_q, bytes_q, q_recv.at[rd]).wait()
        sums = [jnp.sum(qb[rd, pl.ds(d * nc, nc)], axis=0) for d in range(nb)]
        band = [jnp.broadcast_to(sums[d // 2][d % 2 : d % 2 + 1], (rows, lanes)) for d in range(nr)]
        cols = {}

        def column(k, d):
            return lane_sum(band[d] * kt[k])

        gamma = curve = None
        if want_dots:
            cross = jnp.zeros((rows, lanes), jnp.float32)
            for d in range(nr):
                total = jnp.zeros((rows, lanes), jnp.float32)
                if ndev <= UNROLL:
                    for e in range(nc):
                        cols[(d, e)] = column(d * nc + e, d)
                        total = total + jnp.where(place(e), cols[(d, e)], 0.0)
                else:
                    def add(e, total):
                        return total + jnp.where(place(e), column(d * nc + e, d), 0.0)
                    total = lax.fori_loop(0, nc, add, total)
                cross = cross + total * band[d]
            everything = functools.reduce(jnp.add, band)
            crossed = jnp.broadcast_to(jnp.sum(cross, axis=0, keepdims=True), (rows, lanes))
            curve = lane_sum(jnp.where(of_rhs, crossed, 0.0) + jnp.where(curve_lane, everything, 0.0))
            gamma = lane_sum(jnp.where(gamma_lane, everything, 0.0))
        turned = {}
        for at in keys:
            if at not in cols:
                cols[at] = column(at[0] * nc + at[1], at[0])
            wide_col = jnp.broadcast_to(cols[at], (rows, width))
            for m in range(sc):
                turned[at, m] = pltpu.roll(wide_col, m * nrhs, 0) if m else wide_col
        return turned, gamma, curve

    def beside(a):
        return [key(a, 1), key(2, 0) if a else key(-1, 0)]

    def precondition(images):
        weighted = []
        for a in range(2):
            total = images[key(a, 0)].shape[0]
            ring = multiply(jnp.concatenate([images[at] for at in beside(a)], axis=0), fpair[a])
            weighted.append({at: ring[m * total : (m + 1) * total] for m, at in enumerate(beside(a))})
            weighted[a][key(a, -1)] = weighted[a][key(a, 1)]
        for a in range(2):
            mine = multiply(images[key(a, 0)], dpair[a])
            for ring in weighted:
                ring[key(a, 0)] = mine
        return weighted

    def jump_sides(tiles, a):
        east, mine, west = (tiles[key(a, dj)] for dj in (1, 0, -1))
        before = jnp.where(row < rows - nrhs, west, mine)
        after = jnp.where(row < nrhs, mine, east)
        flat = [jnp.where(row < nrhs, tiles.get(key(a + d, 1), east), tiles.get(key(a + d, -1), west)) for d in (-1, 1)]
        return meet(jnp.where(row < nrhs, east, west), before, after, *flat, a, side_lookups[a])

    def images_of(tiles):
        images = {key(*near[n]): jump_at(tiles, *near[n], lookups[n]) for n in (0, 1, SOUTH, NORTH)}
        for a in range(2):
            images[key(a, 1)] = jump_sides(tiles, a)
        return images

    def advance(tiles, keep):
        if not keep:
            return [jump_at(tiles, a, 0, lookups[a]) for a in range(2)], None
        images = images_of(tiles)
        weighted = precondition(images)
        step = [jump_at(weighted[a], a, 0, lookups[a]) for a in range(2)]
        return [images[key(a, 0)] for a in range(2)], step

    def lift(step):
        return [multiply(step[a], lpair[a]) for a in range(2)]

    def coarse(table, turned):
        sums = []
        for a in range(2):
            terms = [table[a][at, m] * turned[at, m] for at, m in table[a]]
            while len(terms) > 1:
                terms = [sum(terms[k + 1 : k + 2], terms[k]) for k in range(0, len(terms), 2)]
            sums.append(terms[0])
        return sums

    arrived(LINV)
    for a in range(2):
        split_into(lpair.at[a], [2.0 * lbuf[a, s] for s in range(sc)])
        fpair[a] = jnp.zeros(fpair.shape[1:], jnp.bfloat16)

    arrived(PAIR_PART)
    arrived(PAIR_CPL)
    partners = [spread(part_n[n]) for n in range(2)]
    lookups = [partner > 0.5 for partner in partners]
    couplings = {(a, 0): spread(cpl_n[a]) for a in range(2)}
    arrived(LOADS)
    load_tiles = {key(*at): loads_n[n] for n, at in enumerate(near)}
    start = [jump_at(load_tiles, a, 0, lookups[a]) for a in range(2)]
    publish(0, start, [multiply(0.5 * start[a], lpair[a]) for a in range(2)], None)

    arrived(PART)
    partners += [spread(part_n[n]) for n in range(2, len(near))]
    lookups += [partner > 0.5 for partner in partners[2:]]
    side_lookups = [jnp.where(row < nrhs, partners[EAST + a], partners[WEST + a]) > 0.5 for a in range(2)]
    arrived(CPL)
    for at, (n, a) in keys.items():
        if n:
            couplings[at] = spread(cpl_n[2 * n + a])
    arrived(SIDE)
    arrived(FLAT)
    arrived(DIRICH)

    def edge_into(block, a, s, first):
        high, low = split(2.0 * block.T)
        fpair[a, s * width : (s + 1) * width, first : first + edge] = high
        fpair[a, s * width : (s + 1) * width, width + first : width + first + edge] = low

    for a in range(2):
        split_into(dpair.at[a], [2.0 * dbuf[a, s] for s in range(sc)])
        edge_into(dside[a], a, 0, edge * (1 - (a + sc - 1) % 2))
        edge_into(dside[2 + a], a, sc - 1, edge * (a % 2))
        for s in range(sc):
            edge_into(dflat[a, s], a, s, edge * (2 + s % 2))

    group = nrhs // sc
    order = list(keys)
    nothing = jnp.zeros((rows, width), jnp.float32)
    batches = [order[first : first + group] for first in range(0, len(order), group)]
    basis_images = []
    for batch in batches:
        tiles = {at: nothing for at in order}
        for g, at in enumerate(batch):
            tiles[at] = jnp.where(rhs_row == g * sc + sub_row, couplings[at], 0.0)
        basis_images.append(images_of(tiles))
    stacked = {at: jnp.concatenate([images[at] for images in basis_images], axis=0) for at in basis_images[0]}
    basis_weighted = precondition(stacked)
    stacked_steps = []
    for a in range(2):
        parts = [
            jump_at({at: basis_weighted[a][at][b * rows : (b + 1) * rows] for at in basis_weighted[a]}, a, 0, lookups[a])
            for b in range(len(batches))
        ]
        stacked_steps.append(jnp.concatenate(parts, axis=0))
    stacked_u = [multiply(stacked_steps[a], lpair[a]) for a in range(2)]

    def table_of(stacks, farthest):
        tables = []
        for a, stack in enumerate(stacks):
            table = {}
            for n, at in enumerate(order):
                if reach(a, at) > farthest:
                    continue
                first = (n // group) * rows + (n % group) * sc
                for m in range(sc):
                    value = None
                    for s in range(sc):
                        at_row = first + s * nrhs + (s - m) % sc
                        line = jnp.broadcast_to(stack[at_row : at_row + 1], (rows, width))
                        value = line if value is None else jnp.where(sub_row == s, line, value)
                    table[at, m] = value
            tables.append(table)
        return tables

    image_table = table_of([stacked[key(a, 0)] for a in range(2)], 1)
    step_table = table_of(stacked_steps, 2)
    u_table = table_of(stacked_u, 2)

    arrived(KROW)

    def widen(k):
        kt[k] = jnp.where(of_rhs, spread(kc[k]), 0.0)

    if ndev <= UNROLL:
        for k in range(ndev):
            widen(k)
    else:
        pl.loop(0, ndev)(widen)

    def pairwise(function, *operands):
        return [function(*(operand[a] for operand in operands)) for a in range(2)]

    def plus(left, right):
        return pairwise(jnp.add, left, right)

    image, step = advance(collect_tiles(0), True)
    turned, _, _ = collect_sums(0, False)
    lifted = lift(step)
    residual = plus(image, coarse(image_table, turned))
    precon = plus(step, coarse(step_table, turned))
    u = plus(lifted, coarse(u_table, turned))

    multipliers = [nothing, nothing]
    search = along = steps = lifts = gamma = step_size = ratio = None
    for iteration in range(ITERS):
        rd = iteration + 1
        last = rd == ITERS
        doubled = [2.0 * value for value in precon]
        dots = (residual[0] * precon[0] + residual[1] * precon[1], doubled[0] * u[0] + doubled[1] * u[1])
        publish(rd, doubled, u, dots)
        if iteration == 0:
            for what in arrivals:
                left(what)
        sent(rd - 1)
        if last:
            sent(rd)
        image, step = advance(collect_tiles(rd), not last)
        turned, gamma_new, curve = collect_sums(rd, True)
        if iteration == 0:
            step_size = gamma_new / curve
            search = precon
        else:
            ratio = gamma_new / gamma
            step_size = gamma_new / (curve - ratio * gamma_new / step_size)
            search = pairwise(lambda new, old: new + ratio * old, precon, search)

        def known(table, old):
            fixed = coarse(table, turned)
            return fixed if old is None else pairwise(lambda new, before: new + ratio * before, fixed, old)

        def descend(value, fixed, new):
            return pairwise(lambda v, f, n: (v - step_size * f) - step_size * n, value, fixed, new)

        gamma = gamma_new
        multipliers = pairwise(lambda value, move: value + step_size * move, multipliers, search)
        fixed = known(image_table, along)
        residual = descend(residual, fixed, image)
        along = plus(image, fixed)
        if not last:
            fixed = known(step_table, steps)
            precon = descend(precon, fixed, step)
            steps = plus(step, fixed)
            fixed = known(u_table, lifts)
            lifted = lift(step)
            u = descend(u, fixed, lifted)
            lifts = plus(lifted, fixed)
    first_row = jnp.full((rows, width), core, jnp.int32) == 0
    out[0] = pick(jnp.where(first_row, multipliers[0], multipliers[1]), backward)
    out[1] = pick(jnp.where(first_row, residual[0], residual[1]), backward)


def solution(mesh):
    nr, nc = mesh.shape["srow"], mesh.shape["scol"]
    slots = block_slots(nr // 2, nc)

    def body(loads, local_inverse, dirichlet, corner_coupling, coarse_inverse, partner):
        sr, sc, nrhs, width = loads.shape
        rows = sr * sc * nrhs
        ndev = nr * nc
        lanes = -(-(nrhs * nc * sc + 2 * nrhs) // 128) * 128
        dma = pltpu.SemaphoreType.DMA
        f32 = jnp.float32
        vmem = pl.BlockSpec(memory_space=pltpu.VMEM)
        hbm = pl.BlockSpec(memory_space=pl.ANY)
        rounds = ITERS + 1
        edge = width // 4
        out = pl.pallas_call(
            functools.partial(kernel, nr, nc, slots, sc, nrhs),
            out_shape=pltpu.VMEM((2, rows, width), f32),
            in_specs=[hbm] * 6,
            out_specs=vmem,
            scratch_shapes=[
                pltpu.VMEM((sc, coarse_inverse.shape[-1]), f32),
                pltpu.VMEM((rows, width), f32),
                pltpu.VMEM((sc, width), f32),
                pltpu.VMEM((sc, width), jnp.int32),
                pltpu.VMEM((2, sc, width, width), f32),
                pltpu.VMEM((2, sc, width, width), f32),
                pltpu.VMEM((2, sc * width, 2 * width), jnp.bfloat16),
                pltpu.VMEM((2, sc * width, 2 * width), jnp.bfloat16),
                pltpu.VMEM((2, sc * width, 2 * width), jnp.bfloat16),
                pltpu.VMEM((8, rows, width), f32),
                pltpu.VMEM((8, sc, width), f32),
                pltpu.VMEM((2 * len(slots), sc, width), f32),
                pltpu.VMEM((4, edge, width), f32),
                pltpu.VMEM((2, sc, edge, width), f32),
                pltpu.VMEM((ndev, sc, lanes), f32),
                pltpu.VMEM((ndev, rows, lanes), f32),
                pltpu.VMEM((rounds, len(slots), 2, rows, width), f32),
                pltpu.VMEM((rounds, ndev // 2, 2, lanes), f32),
                dma((6,)), dma((10,)), dma((10,)),
                dma((rounds,)), dma((rounds,)),
                dma((rounds,)), dma((rounds,)),
            ],
            compiler_params=pltpu.CompilerParams(collective_id=0, has_side_effects=True),
        )(
            loads.reshape(rows, width),
            corner_coupling.reshape(sc, width),
            coarse_inverse.reshape(sc, coarse_inverse.shape[-1]),
            partner.reshape(sc, width),
            local_inverse.reshape(sc, width, width),
            dirichlet.reshape(sc, width, width),
        )
        return out[0].reshape(loads.shape), out[1].reshape(loads.shape)

    whole, lists = P("srow", "scol", None, None), P("srow", "scol", None)
    return jax.shard_map(
        body,
        mesh=mesh,
        in_specs=(whole, whole, whole, lists, lists, lists),
        out_specs=(whole, whole),
        check_vma=False,
    )
```

```python
import functools

import jax
import jax.numpy as jnp
from jax import lax
from jax.experimental import pallas as pl
from jax.experimental.pallas import tpu as pltpu
from jax.sharding import PartitionSpec as P

ITERS = 3
MESH = pl.DeviceIdType.MESH
precise = lax.Precision.HIGHEST
UNROLL = 64
EAST, WEST, SOUTH, NORTH = 2, 4, 6, 7


def block_slots(nb, nc):
    slots = []
    for dp, dj in ((0, 0), (0, 1), (0, -1), (1, 0), (-1, 0), (1, 1), (1, -1), (-1, 1), (-1, -1)):
        off = (dp % nb, dj % nc)
        if off not in slots:
            slots.append(off)
    return slots


def kernel(nr, nc, slots, sc, nrhs, loads_in, cpl_in, cinv_in, part_in, linv, dirich, out,
           cinv, loads, cpl, part, lbuf, dbuf, lpair, dpair, fpair, loads_n, part_n, cpl_n, dside, dflat, kc, kt, ub, qb,
           local_sem, send_sem, recv_sem, u_send, u_recv, q_send, q_recv):
    rows, width = loads_n.shape[1:]
    edge = width // 4
    ndev = nr * nc
    nb = nr // 2
    nblocks = nb * nc
    ncols = nc * sc
    lanes = kt.shape[-1]
    i, j = lax.axis_index("srow"), lax.axis_index("scol")
    p, core = lax.div(i, 2), lax.rem(i, 2)
    near = [(0, 0), (1, 0), (0, 1), (1, 1), (0, nc - 1), (1, nc - 1), (nr - 1, 0), (2, 0)]
    LOADS, PART, CPL, LINV, DIRICH, SIDE, FLAT, KROW, PAIR_PART, PAIR_CPL = range(10)

    def flip(index, mask):
        for bit in range(mask.bit_length()):
            if mask >> bit & 1:
                index = index + (1 << bit) - (2 << bit) * lax.rem(lax.div(index, 1 << bit), 2)
        return index

    powers = nb & (nb - 1) == 0 and nc & (nc - 1) == 0
    masks = sorted(((a, b) for a in range(nb) for b in range(nc) if a or b), key=lambda m: -(m[0] + m[1] // 2 + m[1] % 2))

    paired = ndev <= UNROLL and powers
    rows_to = [flip(i, 2 * a + c) for a in range(nb) for c in range(2)] if paired else []
    cols_to = [flip(j, b) for b in range(nc)] if paired else []

    def others(step):
        if paired:
            for a, b in [*masks, (0, 0)]:
                for c in range(2):
                    if a or b or c:
                        step(rows_to[2 * a + c], cols_to[b])
        elif ndev <= UNROLL:
            for k in range(1, ndev):
                step(lax.rem(i + k // nc, nr), lax.rem(j + k % nc, nc))
        else:
            @pl.loop(1, ndev)
            def _(k):
                step(lax.rem(i + lax.div(k, nc), nr), lax.rem(j + lax.rem(k, nc), nc))

    barrier = pltpu.get_barrier_semaphore()

    def greet(ti, tj):
        pl.semaphore_signal(barrier, inc=1, device_id=(ti, tj), device_id_type=MESH)

    fetches = [
        pltpu.make_async_copy(src, dst, local_sem.at[n])
        for n, (src, dst) in enumerate((
            (loads_in, loads), (part_in, part), (cpl_in, cpl), (cinv_in, cinv),
            (linv, lbuf.at[core]), (dirich, dbuf.at[core]),
        ))
    ]
    for fetch in fetches[:2]:
        fetch.start()
    others(greet)
    for fetch in fetches[2:]:
        fetch.start()

    row = lax.broadcasted_iota(jnp.int32, (rows, width), 0)
    lane = lax.broadcasted_iota(jnp.int32, (rows, width), 1)
    wrow = lax.broadcasted_iota(jnp.int32, (rows, lanes), 0)
    wlane = lax.broadcasted_iota(jnp.int32, (rows, lanes), 1)
    wrhs = lax.rem(wrow, nrhs)
    wsub = lax.div(wrow, nrhs)
    of_rhs = lax.div(wlane, ncols) == wrhs
    gamma_lane = wlane == nrhs * ncols + wrhs
    curve_lane = wlane == nrhs * ncols + nrhs + wrhs
    rhs_row = lax.rem(row, nrhs)
    sub_row = lax.div(row, nrhs)

    def spread(block):
        out = jnp.broadcast_to(block[0:1], (rows, block.shape[1]))
        which = lax.div(lax.broadcasted_iota(jnp.int32, out.shape, 0), nrhs)
        for s in range(1, sc):
            out = jnp.where(which == s, jnp.broadcast_to(block[s : s + 1], out.shape), out)
        return out

    def place(dj):
        column = lax.rem(j + dj, nc) * sc
        return wlane == wrhs * ncols + column + wsub

    def pick(values, index):
        return jnp.take_along_axis(values, index, axis=1, mode="promise_in_bounds")

    side = lax.div(lane, edge)
    half = lax.rem(side, 2)

    def odd(dr):
        return lax.rem(sub_row + dr, 2)

    def split(values):
        high = values.astype(jnp.bfloat16)
        return high, (values - high.astype(jnp.float32)).astype(jnp.bfloat16)

    def split_into(pair, blocks):
        for s, block in enumerate(blocks):
            high, low = split(block)
            pair[s * width : (s + 1) * width, 0:width] = high
            pair[s * width : (s + 1) * width, width : 2 * width] = low

    for fetch in fetches[:2]:
        fetch.wait()
    partner = spread(part[...])
    other = edge * (1 - 2 * half)
    mirrored = jnp.where((half == 1) & (partner >= 0), partner + side * edge, lane)
    crossed_over = jnp.where(half == 0, pltpu.roll(mirrored, width - edge, 1), pltpu.roll(mirrored, edge, 1))
    own_odd = odd(core)
    forward = jnp.where(own_odd == 1, crossed_over, mirrored)
    backward = jnp.where(own_odd == 1, mirrored + other, mirrored)
    loads_n[core] = pick(loads[...], forward)
    active_own = pick(jnp.where(partner >= 0, 1.0, 0.0), forward)
    for s in range(sc):
        part_n[core, s : s + 1] = active_own[s * nrhs : s * nrhs + 1]

    def reorder(buffer):
        for s in range(sc):
            index = jnp.broadcast_to(forward[s * nrhs : s * nrhs + 1], (width, width))
            buffer[core, s] = pick(pick(buffer[core, s], index).T, index)

    pl.semaphore_wait(barrier, ndev - 1)

    def push(src, dst, what, ti, tj):
        pltpu.make_async_remote_copy(
            src_ref=src, dst_ref=dst, send_sem=send_sem.at[what], recv_sem=recv_sem.at[what],
            device_id=(ti, tj), device_id_type=MESH).start()

    west_j, east_j = lax.rem(j + nc - 1, nc), lax.rem(j + 1, nc)
    beyond = lax.rem(p + 2 * core - 1 + nb, nb)
    partner_i = i + 1 - 2 * core
    around = [(EAST + core, 2 * p + t, west_j) for t in range(2)] + [(WEST + core, 2 * p + t, east_j) for t in range(2)]
    around += [(NORTH - core, 2 * beyond + t, j) for t in range(2)]
    toward = around + [(core, partner_i, j)]
    for n, ti, tj in toward:
        push(loads_n.at[core], loads_n.at[n], LOADS, ti, tj)
    push(part_n.at[core], part_n.at[core], PAIR_PART, partner_i, j)
    for n, ti, tj in around:
        push(part_n.at[core], part_n.at[n], PART, ti, tj)
    fetches[2].wait()
    coupling_own = pick(spread(cpl[...]), forward)
    for s in range(sc):
        cpl_n[core, s : s + 1] = coupling_own[s * nrhs : s * nrhs + 1]
    push(cpl_n.at[core], cpl_n.at[core], PAIR_CPL, partner_i, j)
    for n, (dp, dj) in enumerate(slots):
        for t in range(2):
            ti, tj = 2 * lax.rem(p - dp + nb, nb) + t, lax.rem(j - dj + nc, nc)
            if n:
                push(cpl_n.at[core], cpl_n.at[2 * n + core], CPL, ti, tj)
    tile_lane = lax.broadcasted_iota(jnp.int32, (ncols, lanes), 1)
    tile_row = lax.broadcasted_iota(jnp.int32, (ncols, lanes), 0)
    tiler = jnp.where(lax.rem(tile_lane, ncols) == tile_row, 1.0, 0.0)
    fetches[3].wait()
    tiled = jnp.dot(spread(cinv[...]), tiler, precision=precise, preferred_element_type=jnp.float32)
    for s in range(sc):
        kc[core * nc, s : s + 1] = tiled[s * nrhs : s * nrhs + 1]
    own_place = place(0)
    def send_k(ti, tj):
        slot = lax.rem(i - 2 * lax.div(ti, 2) + nr, nr) * nc + lax.rem(j - tj + nc, nc)
        push(kc.at[core * nc], kc.at[slot], KROW, ti, tj)

    others(send_k)
    fetches[4].wait()
    reorder(lbuf)
    push(lbuf.at[core], lbuf.at[core], LINV, partner_i, j)
    fetches[5].wait()
    reorder(dbuf)

    def facing_rows(s, group):
        return dbuf.at[core, s, pl.ds(pl.multiple_of(group * edge, edge), edge)]

    for n, ti, tj in around[:2]:
        push(facing_rows(0, lax.rem(core, 2)), dside.at[core], SIDE, ti, tj)
    for n, ti, tj in around[2:4]:
        push(facing_rows(sc - 1, 1 - lax.rem(core + sc - 1, 2)), dside.at[2 + core], SIDE, ti, tj)
    for n, ti, tj in around[4:]:
        for s in range(sc):
            push(facing_rows(s, 2 + s % 2), dflat.at[1 - core, s], FLAT, ti, tj)
    push(dbuf.at[core], dbuf.at[core], DIRICH, partner_i, j)

    arrivals = {
        LOADS: loads_n.at[pl.ds(0, 7)], PART: part_n.at[pl.ds(0, 6)], CPL: cpl_n.at[pl.ds(0, 2 * len(slots) - 2)],
        PAIR_PART: part_n.at[0], PAIR_CPL: cpl_n.at[0],
        LINV: lbuf.at[0], DIRICH: dbuf.at[0], SIDE: dside, FLAT: dflat, KROW: kc.at[pl.ds(0, ndev - 1)],
    }

    def arrived(what):
        pltpu.make_async_copy(arrivals[what], arrivals[what], recv_sem.at[what]).wait()

    def left(what):
        pltpu.make_async_copy(arrivals[what], arrivals[what], send_sem.at[what]).wait()

    def meet(mine, before, after, south, north, dr, active):
        if rows == 2 * nrhs:
            lateral = pltpu.roll(jnp.where(half == odd(dr + 1), before, after), nrhs, 0)
        else:
            lateral = jnp.where(half == odd(dr), pltpu.roll(before, nrhs, 0), pltpu.roll(after, rows - nrhs, 0))
        facing = jnp.where(side < 2, lateral, jnp.where(half == odd(dr), south, north))
        return jnp.where(active, mine - facing, 0.0)

    def jump(mine, west_tile, east_tile, south, north, dr, active):
        before = jnp.where(row < rows - nrhs, mine, west_tile)
        after = jnp.where(row < nrhs, east_tile, mine)
        return meet(mine, before, after, south, north, dr, active)

    def key(dr, dj):
        return (dr % nr, dj % nc)

    def jump_at(tiles, dr, dj, lookup):
        mine = tiles[key(dr, dj)]
        beyond = [tiles.get(key(*at), mine) for at in ((dr, dj - 1), (dr, dj + 1), (dr - 1, dj), (dr + 1, dj))]
        return jump(mine, *beyond, dr, lookup)

    def multiply(values, pair):
        total = values.shape[0]
        high = values.astype(jnp.bfloat16).astype(jnp.float32)
        stacked = jnp.concatenate([high, values - high], axis=0)
        sub = lax.rem(lax.div(lax.broadcasted_iota(jnp.int32, stacked.shape, 0), nrhs), sc)
        wide = jnp.concatenate([jnp.where(sub == s, stacked, 0.0) for s in range(sc)], axis=1)
        product = jnp.dot(wide.astype(jnp.bfloat16), pair, preferred_element_type=jnp.float32)
        return (product[0:total, 0:width] + product[total:, 0:width]) + (product[0:total, width:] + product[total:, width:])

    def lane_sum(values):
        return jnp.sum(values, axis=1, keepdims=True)

    keys = {key(2 * dp + a, dj): (n, a) for n, (dp, dj) in enumerate(slots) for a in range(2)}

    def reach(a, at):
        return min((at[0] - a) % nr, (a - at[0]) % nr) + min(at[1], nc - at[1])

    def q_target(tp, tj):
        return lax.rem(p - tp + nb, nb) * nc + lax.rem(j - tj + nc, nc), 2 * tp + 1 - core, tj

    q_targets = []
    if nblocks <= UNROLL:
        for a, b in masks:
            q_targets.append(q_target(flip(p, a), flip(j, b)) if powers else q_target(lax.rem(p + a, nb), lax.rem(j + b, nc)))
    u_targets = [
        (n, 2 * lax.rem(p - dp + nb, nb) + 1 - core, lax.rem(j - dj + nc, nc)) for n, (dp, dj) in enumerate(slots) if n
    ]
    u_targets.sort(key=lambda target: (slots[target[0]][1] == 0, slots[target[0]][0] == 0))

    def publish(rd, values, u, dots):
        for a in range(2):
            ub[rd, 0, a] = u[a]

        def across(src, dst, send, recv, ti, tj):
            pltpu.make_async_remote_copy(
                src_ref=src, dst_ref=dst, send_sem=send.at[rd], recv_sem=recv.at[rd],
                device_id=(ti, tj), device_id_type=MESH).start()

        for n, ti, tj in [target for target in u_targets if target[0] < reached(rd)]:
            across(ub.at[rd, 0], ub.at[rd, n], u_send, u_recv, ti, tj)
        for a in range(2):
            message = jnp.where(own_place, lane_sum(couplings[a, 0] * values[a]), 0.0)
            if dots is not None and a == 0:
                gamma, curve = dots
                message = jnp.where(gamma_lane, lane_sum(gamma), message)
                message = jnp.where(curve_lane, lane_sum(curve), message)
            qb[rd, 0, a : a + 1] = jnp.sum(message, axis=0, keepdims=True)
        if nblocks <= UNROLL:
            for slot, ti, tj in q_targets:
                across(qb.at[rd, 0], qb.at[rd, slot], q_send, q_recv, ti, tj)
        else:
            @pl.loop(1, nblocks)
            def _(k):
                slot, ti, tj = q_target(lax.rem(p + lax.div(k, nc), nb), lax.rem(j + lax.rem(k, nc), nc))
                across(qb.at[rd, 0], qb.at[rd, slot], q_send, q_recv, ti, tj)

    straight = sum(1 for dp, dj in slots if not dp or not dj)

    def reached(rd):
        return straight if rd == ITERS else len(slots)

    def sent(rd):
        bytes_q = qb.at[rd, pl.ds(1, nblocks - 1)]
        pltpu.make_async_copy(bytes_q, bytes_q, q_send.at[rd]).wait()
        bytes_u = ub.at[rd, pl.ds(1, reached(rd) - 1)]
        pltpu.make_async_copy(bytes_u, bytes_u, u_send.at[rd]).wait()

    def collect_tiles(rd):
        bytes_u = ub.at[rd, pl.ds(1, reached(rd) - 1)]
        pltpu.make_async_copy(bytes_u, bytes_u, u_recv.at[rd]).wait()
        return {at: ub[rd, n, a] for at, (n, a) in keys.items() if n < reached(rd)}

    def collect_sums(rd, want_dots):
        bytes_q = qb.at[rd, pl.ds(1, nblocks - 1)]
        pltpu.make_async_copy(bytes_q, bytes_q, q_recv.at[rd]).wait()
        sums = [jnp.sum(qb[rd, pl.ds(d * nc, nc)], axis=0) for d in range(nb)]
        band = [jnp.broadcast_to(sums[d // 2][d % 2 : d % 2 + 1], (rows, lanes)) for d in range(nr)]
        cols = {}

        def column(k, d):
            return lane_sum(band[d] * kt[k])

        gamma = curve = None
        if want_dots:
            cross = jnp.zeros((rows, lanes), jnp.float32)
            for d in range(nr):
                total = jnp.zeros((rows, lanes), jnp.float32)
                if ndev <= UNROLL:
                    for e in range(nc):
                        cols[(d, e)] = column(d * nc + e, d)
                        total = total + jnp.where(place(e), cols[(d, e)], 0.0)
                else:
                    def add(e, total):
                        return total + jnp.where(place(e), column(d * nc + e, d), 0.0)
                    total = lax.fori_loop(0, nc, add, total)
                cross = cross + total * band[d]
            everything = functools.reduce(jnp.add, band)
            crossed = jnp.broadcast_to(jnp.sum(cross, axis=0, keepdims=True), (rows, lanes))
            curve = lane_sum(jnp.where(of_rhs, crossed, 0.0) + jnp.where(curve_lane, everything, 0.0))
            gamma = lane_sum(jnp.where(gamma_lane, everything, 0.0))
        turned = {}
        for at in keys:
            if at not in cols:
                cols[at] = column(at[0] * nc + at[1], at[0])
            wide_col = jnp.broadcast_to(cols[at], (rows, width))
            for m in range(sc):
                turned[at, m] = pltpu.roll(wide_col, m * nrhs, 0) if m else wide_col
        return turned, gamma, curve

    def beside(a):
        return [key(a, 1), key(2, 0) if a else key(-1, 0)]

    def precondition(images):
        weighted = []
        for a in range(2):
            total = images[key(a, 0)].shape[0]
            ring = multiply(jnp.concatenate([images[at] for at in beside(a)], axis=0), fpair[a])
            weighted.append({at: ring[m * total : (m + 1) * total] for m, at in enumerate(beside(a))})
            weighted[a][key(a, -1)] = weighted[a][key(a, 1)]
        for a in range(2):
            mine = multiply(images[key(a, 0)], dpair[a])
            for ring in weighted:
                ring[key(a, 0)] = mine
        return weighted

    def jump_sides(tiles, a):
        east, mine, west = (tiles[key(a, dj)] for dj in (1, 0, -1))
        before = jnp.where(row < rows - nrhs, west, mine)
        after = jnp.where(row < nrhs, mine, east)
        flat = [jnp.where(row < nrhs, tiles.get(key(a + d, 1), east), tiles.get(key(a + d, -1), west)) for d in (-1, 1)]
        return meet(jnp.where(row < nrhs, east, west), before, after, *flat, a, side_lookups[a])

    def images_of(tiles):
        images = {key(*near[n]): jump_at(tiles, *near[n], lookups[n]) for n in (0, 1, SOUTH, NORTH)}
        for a in range(2):
            images[key(a, 1)] = jump_sides(tiles, a)
        return images

    def advance(tiles, keep):
        if not keep:
            return [jump_at(tiles, a, 0, lookups[a]) for a in range(2)], None
        images = images_of(tiles)
        weighted = precondition(images)
        step = [jump_at(weighted[a], a, 0, lookups[a]) for a in range(2)]
        return [images[key(a, 0)] for a in range(2)], step

    def lift(step):
        return [multiply(step[a], lpair[a]) for a in range(2)]

    def coarse(table, turned):
        sums = []
        for a in range(2):
            terms = [table[a][at, m] * turned[at, m] for at, m in table[a]]
            while len(terms) > 1:
                terms = [sum(terms[k + 1 : k + 2], terms[k]) for k in range(0, len(terms), 2)]
            sums.append(terms[0])
        return sums

    arrived(LINV)
    for a in range(2):
        split_into(lpair.at[a], [2.0 * lbuf[a, s] for s in range(sc)])
        fpair[a] = jnp.zeros(fpair.shape[1:], jnp.bfloat16)

    arrived(PAIR_PART)
    arrived(PAIR_CPL)
    partners = [spread(part_n[n]) for n in range(2)]
    lookups = [partner > 0.5 for partner in partners]
    couplings = {(a, 0): spread(cpl_n[a]) for a in range(2)}
    arrived(LOADS)
    load_tiles = {key(*at): loads_n[n] for n, at in enumerate(near)}
    start = [jump_at(load_tiles, a, 0, lookups[a]) for a in range(2)]
    publish(0, start, [multiply(0.5 * start[a], lpair[a]) for a in range(2)], None)

    arrived(PART)
    partners += [spread(part_n[n]) for n in range(2, len(near))]
    lookups += [partner > 0.5 for partner in partners[2:]]
    side_lookups = [jnp.where(row < nrhs, partners[EAST + a], partners[WEST + a]) > 0.5 for a in range(2)]
    arrived(CPL)
    for at, (n, a) in keys.items():
        if n:
            couplings[at] = spread(cpl_n[2 * n + a])
    arrived(SIDE)
    arrived(FLAT)
    arrived(DIRICH)

    def edge_into(block, a, s, first):
        high, low = split(2.0 * block.T)
        fpair[a, s * width : (s + 1) * width, first : first + edge] = high
        fpair[a, s * width : (s + 1) * width, width + first : width + first + edge] = low

    for a in range(2):
        split_into(dpair.at[a], [2.0 * dbuf[a, s] for s in range(sc)])
        edge_into(dside[a], a, 0, edge * (1 - (a + sc - 1) % 2))
        edge_into(dside[2 + a], a, sc - 1, edge * (a % 2))
        for s in range(sc):
            edge_into(dflat[a, s], a, s, edge * (2 + s % 2))

    group = nrhs // sc
    order = list(keys)
    nothing = jnp.zeros((rows, width), jnp.float32)
    batches = [order[first : first + group] for first in range(0, len(order), group)]
    basis_images = []
    for batch in batches:
        tiles = {at: nothing for at in order}
        for g, at in enumerate(batch):
            tiles[at] = jnp.where(rhs_row == g * sc + sub_row, couplings[at], 0.0)
        basis_images.append(images_of(tiles))
    stacked = {at: jnp.concatenate([images[at] for images in basis_images], axis=0) for at in basis_images[0]}
    basis_weighted = precondition(stacked)
    stacked_steps = []
    for a in range(2):
        parts = [
            jump_at({at: basis_weighted[a][at][b * rows : (b + 1) * rows] for at in basis_weighted[a]}, a, 0, lookups[a])
            for b in range(len(batches))
        ]
        stacked_steps.append(jnp.concatenate(parts, axis=0))
    stacked_u = [multiply(stacked_steps[a], lpair[a]) for a in range(2)]

    def table_of(stacks, farthest):
        tables = []
        for a, stack in enumerate(stacks):
            table = {}
            for n, at in enumerate(order):
                if reach(a, at) > farthest:
                    continue
                first = (n // group) * rows + (n % group) * sc
                for m in range(sc):
                    value = None
                    for s in range(sc):
                        at_row = first + s * nrhs + (s - m) % sc
                        line = jnp.broadcast_to(stack[at_row : at_row + 1], (rows, width))
                        value = line if value is None else jnp.where(sub_row == s, line, value)
                    table[at, m] = value
            tables.append(table)
        return tables

    image_table = table_of([stacked[key(a, 0)] for a in range(2)], 1)
    step_table = table_of(stacked_steps, 2)
    u_table = table_of(stacked_u, 2)

    arrived(KROW)

    def widen(k):
        kt[k] = jnp.where(of_rhs, spread(kc[k]), 0.0)

    if ndev <= UNROLL:
        for k in range(ndev):
            widen(k)
    else:
        pl.loop(0, ndev)(widen)

    def pairwise(function, *operands):
        return [function(*(operand[a] for operand in operands)) for a in range(2)]

    def plus(left, right):
        return pairwise(jnp.add, left, right)

    image, step = advance(collect_tiles(0), True)
    turned, _, _ = collect_sums(0, False)
    lifted = lift(step)
    residual = plus(image, coarse(image_table, turned))
    precon = plus(step, coarse(step_table, turned))
    u = plus(lifted, coarse(u_table, turned))

    first_row = jnp.full((rows, width), core, jnp.int32) == 0

    def placed(values):
        return pick(jnp.where(first_row, values[0], values[1]), backward)

    multipliers = [nothing, nothing]
    search = along = steps = lifts = gamma = step_size = ratio = None
    for iteration in range(ITERS):
        rd = iteration + 1
        last = rd == ITERS
        doubled = [2.0 * value for value in precon]
        dots = (residual[0] * precon[0] + residual[1] * precon[1], doubled[0] * u[0] + doubled[1] * u[1])
        publish(rd, doubled, u, dots)
        if iteration == 0:
            for what in arrivals:
                left(what)
        sent(rd - 1)
        if last:
            sent(rd)
        image, step = advance(collect_tiles(rd), not last)
        turned, gamma_new, curve = collect_sums(rd, True)
        if iteration == 0:
            step_size = gamma_new / curve
            search = precon
        else:
            ratio = gamma_new / gamma
            step_size = gamma_new / (curve - ratio * gamma_new / step_size)
            old_search = search
            search = pairwise(lambda new, old: new + ratio * old, precon, search)

        def known(table, old):
            fixed = coarse(table, turned)
            return fixed if old is None else pairwise(lambda new, before: new + ratio * before, fixed, old)

        def descend(value, fixed, new):
            return pairwise(lambda v, f, n: (v - step_size * f) - step_size * n, value, fixed, new)

        gamma = gamma_new
        if last:
            move = placed(precon) if ratio is None else placed(precon) + ratio * placed(old_search)
            out[0] = placed(multipliers) + step_size * move
            fixed = placed(coarse(image_table, turned))
            if ratio is not None:
                fixed = fixed + ratio * placed(along)
            out[1] = (placed(residual) - step_size * fixed) - step_size * placed(image)
            break
        multipliers = pairwise(lambda value, move: value + step_size * move, multipliers, search)
        fixed = known(image_table, along)
        residual = descend(residual, fixed, image)
        along = plus(image, fixed)
        if not last:
            fixed = known(step_table, steps)
            precon = descend(precon, fixed, step)
            steps = plus(step, fixed)
            fixed = known(u_table, lifts)
            lifted = lift(step)
            u = descend(u, fixed, lifted)
            lifts = plus(lifted, fixed)


def solution(mesh):
    nr, nc = mesh.shape["srow"], mesh.shape["scol"]
    slots = block_slots(nr // 2, nc)

    def body(loads, local_inverse, dirichlet, corner_coupling, coarse_inverse, partner):
        sr, sc, nrhs, width = loads.shape
        rows = sr * sc * nrhs
        ndev = nr * nc
        lanes = -(-(nrhs * nc * sc + 2 * nrhs) // 128) * 128
        dma = pltpu.SemaphoreType.DMA
        f32 = jnp.float32
        vmem = pl.BlockSpec(memory_space=pltpu.VMEM)
        hbm = pl.BlockSpec(memory_space=pl.ANY)
        rounds = ITERS + 1
        edge = width // 4
        out = pl.pallas_call(
            functools.partial(kernel, nr, nc, slots, sc, nrhs),
            out_shape=pltpu.VMEM((2, rows, width), f32),
            in_specs=[hbm] * 6,
            out_specs=vmem,
            scratch_shapes=[
                pltpu.VMEM((sc, coarse_inverse.shape[-1]), f32),
                pltpu.VMEM((rows, width), f32),
                pltpu.VMEM((sc, width), f32),
                pltpu.VMEM((sc, width), jnp.int32),
                pltpu.VMEM((2, sc, width, width), f32),
                pltpu.VMEM((2, sc, width, width), f32),
                pltpu.VMEM((2, sc * width, 2 * width), jnp.bfloat16),
                pltpu.VMEM((2, sc * width, 2 * width), jnp.bfloat16),
                pltpu.VMEM((2, sc * width, 2 * width), jnp.bfloat16),
                pltpu.VMEM((8, rows, width), f32),
                pltpu.VMEM((8, sc, width), f32),
                pltpu.VMEM((2 * len(slots), sc, width), f32),
                pltpu.VMEM((4, edge, width), f32),
                pltpu.VMEM((2, sc, edge, width), f32),
                pltpu.VMEM((ndev, sc, lanes), f32),
                pltpu.VMEM((ndev, rows, lanes), f32),
                pltpu.VMEM((rounds, len(slots), 2, rows, width), f32),
                pltpu.VMEM((rounds, ndev // 2, 2, lanes), f32),
                dma((6,)), dma((10,)), dma((10,)),
                dma((rounds,)), dma((rounds,)),
                dma((rounds,)), dma((rounds,)),
            ],
            compiler_params=pltpu.CompilerParams(collective_id=0, has_side_effects=True),
        )(
            loads.reshape(rows, width),
            corner_coupling.reshape(sc, width),
            coarse_inverse.reshape(sc, coarse_inverse.shape[-1]),
            partner.reshape(sc, width),
            local_inverse.reshape(sc, width, width),
            dirichlet.reshape(sc, width, width),
        )
        return out[0].reshape(loads.shape), out[1].reshape(loads.shape)

    whole, lists = P("srow", "scol", None, None), P("srow", "scol", None)
    return jax.shard_map(
        body,
        mesh=mesh,
        in_specs=(whole, whole, whole, lists, lists, lists),
        out_specs=(whole, whole),
        check_vma=False,
    )
```
